32 devices in a mesh: rep: 2 (over x), tp: 4 (over z), dp: 4 (over y, core).
Axes of the slice: x: 2, y: 2, z: 4, core: 2. Of those that a mesh axis runs over, the one named last changes fastest.
Arguments:
- x: bfloat16 [256, 2048], P(('rep', 'dp')), parts along dimension 0
- lengths: int32 [256], P(('rep', 'dp')), parts along dimension 0
- cache0: bfloat16 [256, 256, 576], P(('rep', 'dp')), parts along dimension 0
- cache1: bfloat16 [256, 256, 576], P(('rep', 'dp')), parts along dimension 0
- attn_gain: float32 [2, 2048], replicated
- kv_gain: float32 [2, 512], replicated
- q_gain: float32 [2, 1536], replicated
- ffn_gain: float32 [2, 2048], replicated
- w_dkv: bfloat16 [2, 2048, 576], replicated
- w_qa: bfloat16 [2, 2048, 1536], replicated
- w_qb: bfloat16 [2, 1536, 3072], P(None, None, 'tp')
- w_uk: bfloat16 [2, 16, 128, 512], P(None, 'tp')
- w_uv: bfloat16 [2, 16, 512, 128], P(None, 'tp')
- w_o: bfloat16 [2, 2048, 2048], P(None, 'tp')
- w_gate: bfloat16 [2, 2048, 11264], replicated
- w_up: bfloat16 [2, 2048, 11264], replicated
- w_down: bfloat16 [2, 11264, 2048], replicated
Outputs:
- output 1: bfloat16 [256, 2048], P(('rep', 'dp')), parts along dimension 0
- output 2: bfloat16 [256, 256, 576], P(('rep', 'dp')), parts along dimension 0
- output 3: bfloat16 [256, 256, 576], P(('rep', 'dp')), parts along dimension 0
There are 2 independent parts. The reference program is written for one: setup_inputs(seed, part) draws one part's arguments, and reference() takes and returns one part's arrays. A program takes and returns all parts, laid end to end along the dimension named above; an argument that names none is the same for every part.
All inputs are finite; a program needn't handle non-finite values.
Results may differ from the reference program's by a relative error of at most 0.0148903.
Values are sent between devices in bfloat16 or wider.
A program may use at most 1.5 GiB of HBM per device.

```python
import jax
import jax.numpy as jnp
from jax import lax

MODEL_DIM = 2048
FFN_DIM = 11264
NUM_HEADS = 16
Q_LORA = 1536
KV_LORA = 512
ROPE_DIM = 64
NOPE_DIM = 128
V_DIM = 128
BATCH = 128
SEQ_LEN = 256
LAYER_COUNT = 2

LAT_WIDTH = KV_LORA + ROPE_DIM
QK_WIDTH = NOPE_DIM + ROPE_DIM
NORM_EPS = 1e-6
ROPE_BASE = 10000.0


def rms_norm(values, gain_vec):
    wide_vals = values.astype(jnp.float32)
    inv_rms = lax.rsqrt(jnp.mean(wide_vals * wide_vals, axis=-1, keepdims=True) + NORM_EPS)
    return (wide_vals * inv_rms * gain_vec.astype(jnp.float32)).astype(jnp.bfloat16)


def rope_tables(lengths):
    half_dim = ROPE_DIM // 2
    inv_freq = ROPE_BASE ** (-2.0 * jnp.arange(half_dim).astype(jnp.float32) / ROPE_DIM)
    angles = lengths.astype(jnp.float32)[:, None] * inv_freq[None, :]
    return jnp.cos(angles), jnp.sin(angles)


def rotate(values, cos_tab, sin_tab):
    half_dim = values.shape[-1] // 2
    first_half = values[..., :half_dim]
    second_half = values[..., half_dim:]
    return jnp.concatenate([first_half * cos_tab - second_half * sin_tab, second_half * cos_tab + first_half * sin_tab], axis=-1)


def row_attention(row_query, row_cache, row_len):
    scores = jnp.einsum('hk,tk->ht', row_query.astype(jnp.float32), row_cache.astype(jnp.float32)) * QK_WIDTH ** -0.5
    valid_mask = jnp.arange(SEQ_LEN)[None, :] <= row_len
    att_probs = jax.nn.softmax(jnp.where(valid_mask, scores, -1e30), axis=-1).astype(jnp.bfloat16)
    return jnp.einsum('ht,tk->hk', att_probs.astype(jnp.float32), row_cache[:, :KV_LORA].astype(jnp.float32)).astype(jnp.bfloat16)


def layer_step(x_rows, lengths, cache, cos_tab, sin_tab, attn_g, kv_g, q_g, ffn_g, w_dkv, w_qa, w_qb, w_uk, w_uv, w_o, w_gate, w_up, w_down):
    normed = rms_norm(x_rows, attn_g)
    kv_lat = jnp.dot(normed, w_dkv, preferred_element_type=jnp.float32)
    new_entry = jnp.concatenate([rms_norm(kv_lat[:, :KV_LORA], kv_g), rotate(kv_lat[:, KV_LORA:], cos_tab, sin_tab).astype(jnp.bfloat16)], axis=-1)
    is_slot = (jnp.arange(SEQ_LEN)[None, :] == lengths[:, None])[:, :, None]
    new_cache = jnp.where(is_slot, new_entry[:, None, :], cache)
    q_low = rms_norm(jnp.dot(normed, w_qa, preferred_element_type=jnp.float32), q_g)
    q_full = jnp.dot(q_low, w_qb, preferred_element_type=jnp.float32).reshape(BATCH, NUM_HEADS, QK_WIDTH)
    q_nope = q_full[:, :, :NOPE_DIM].astype(jnp.bfloat16)
    q_rot = rotate(q_full[:, :, NOPE_DIM:], cos_tab[:, None, :], sin_tab[:, None, :]).astype(jnp.bfloat16)
    q_lat = jnp.einsum('bhn,hnk->bhk', q_nope.astype(jnp.float32), w_uk.astype(jnp.float32)).astype(jnp.bfloat16)
    query_vec = jnp.concatenate([q_lat, q_rot], axis=-1)
    lat_out = lax.map(lambda row_item: row_attention(row_item[0], row_item[1], row_item[2]), (query_vec, new_cache, lengths))
    head_out = jnp.einsum('bhk,hkv->bhv', lat_out.astype(jnp.float32), w_uv.astype(jnp.float32)).astype(jnp.bfloat16)
    attn_out = jnp.dot(head_out.reshape(BATCH, NUM_HEADS * V_DIM), w_o, preferred_element_type=jnp.float32)
    x_mid = (x_rows.astype(jnp.float32) + attn_out).astype(jnp.bfloat16)
    ffn_in = rms_norm(x_mid, ffn_g)
    hidden = (jax.nn.silu(jnp.dot(ffn_in, w_gate, preferred_element_type=jnp.float32)) * jnp.dot(ffn_in, w_up, preferred_element_type=jnp.float32)).astype(jnp.bfloat16)
    ffn_out = jnp.dot(hidden, w_down, preferred_element_type=jnp.float32)
    return (x_mid.astype(jnp.float32) + ffn_out).astype(jnp.bfloat16), new_cache


def draw_lengths(base_key):
    key_long, key_short, key_pick = jax.random.split(base_key, 3)
    long_len = jax.random.randint(key_long, (BATCH,), 0, SEQ_LEN)
    short_len = jax.random.randint(key_short, (BATCH,), 0, min(4, SEQ_LEN))
    pick_short = jax.random.randint(key_pick, (BATCH,), 0, 2)
    row_ids = jnp.arange(BATCH)
    drawn = jnp.where(pick_short == 1, short_len, long_len)
    drawn = jnp.where(row_ids == 0, SEQ_LEN - 1, drawn)
    drawn = jnp.where(row_ids == 1, 0, drawn)
    return drawn.astype(jnp.int32)


def draw_cache(base_key, lengths):
    key_common, key_noise = jax.random.split(base_key)
    common = jax.random.normal(key_common, (BATCH, 1, LAT_WIDTH), jnp.float32)
    slot_noise = jax.random.normal(key_noise, (BATCH, SEQ_LEN, LAT_WIDTH), jnp.float32)
    filled = (jnp.arange(SEQ_LEN)[None, :] < lengths[:, None])[:, :, None]
    return jnp.where(filled, 0.8 * common + 0.6 * slot_noise, 40.0 * slot_noise).astype(jnp.bfloat16)


def normal_weight(base_key, shape, fan_in):
    return (jax.random.normal(base_key, shape, jnp.float32) * fan_in ** -0.5).astype(jnp.bfloat16)


def setup_inputs(seed: int = 0, part: int = 0) -> dict:
    shared = jax.random.split(jax.random.key(seed), 13)
    part_keys = jax.random.split(jax.random.fold_in(jax.random.key(seed + 1), part), 4)
    lengths = draw_lengths(part_keys[1])
    return {
        'x': jax.random.normal(part_keys[0], (BATCH, MODEL_DIM), jnp.float32).astype(jnp.bfloat16),
        'lengths': lengths,
        'cache0': draw_cache(part_keys[2], lengths),
        'cache1': draw_cache(part_keys[3], lengths),
        'attn_gain': jax.random.uniform(shared[0], (LAYER_COUNT, MODEL_DIM), jnp.float32, 0.4, 1.6),
        'kv_gain': jax.random.uniform(shared[1], (LAYER_COUNT, KV_LORA), jnp.float32, 0.4, 1.6),
        'q_gain': jax.random.uniform(shared[2], (LAYER_COUNT, Q_LORA), jnp.float32, 0.4, 1.6),
        'ffn_gain': jax.random.uniform(shared[3], (LAYER_COUNT, MODEL_DIM), jnp.float32, 0.4, 1.6),
        'w_dkv': normal_weight(shared[4], (LAYER_COUNT, MODEL_DIM, LAT_WIDTH), MODEL_DIM),
        'w_qa': normal_weight(shared[5], (LAYER_COUNT, MODEL_DIM, Q_LORA), MODEL_DIM),
        'w_qb': normal_weight(shared[6], (LAYER_COUNT, Q_LORA, NUM_HEADS * QK_WIDTH), Q_LORA),
        'w_uk': normal_weight(shared[7], (LAYER_COUNT, NUM_HEADS, NOPE_DIM, KV_LORA), NOPE_DIM),
        'w_uv': normal_weight(shared[8], (LAYER_COUNT, NUM_HEADS, KV_LORA, V_DIM), KV_LORA),
        'w_o': normal_weight(shared[9], (LAYER_COUNT, NUM_HEADS * V_DIM, MODEL_DIM), NUM_HEADS * V_DIM),
        'w_gate': normal_weight(shared[10], (LAYER_COUNT, MODEL_DIM, FFN_DIM), MODEL_DIM),
        'w_up': normal_weight(shared[11], (LAYER_COUNT, MODEL_DIM, FFN_DIM), MODEL_DIM),
        'w_down': normal_weight(shared[12], (LAYER_COUNT, FFN_DIM, MODEL_DIM), FFN_DIM // 2),
    }


def reference(x, lengths, cache0, cache1, attn_gain, kv_gain, q_gain, ffn_gain, w_dkv, w_qa, w_qb, w_uk, w_uv, w_o, w_gate, w_up, w_down):
    cos_tab, sin_tab = rope_tables(lengths)
    caches = [cache0, cache1]
    new_caches = []
    x_rows = x
    for layer_idx in range(LAYER_COUNT):
        x_rows, new_cache = layer_step(x_rows, lengths, caches[layer_idx], cos_tab, sin_tab, attn_gain[layer_idx], kv_gain[layer_idx], q_gain[layer_idx], ffn_gain[layer_idx], w_dkv[layer_idx], w_qa[layer_idx], w_qb[layer_idx], w_uk[layer_idx], w_uv[layer_idx], w_o[layer_idx], w_gate[layer_idx], w_up[layer_idx], w_down[layer_idx])
        new_caches.append(new_cache)
    return (x_rows, new_caches[0], new_caches[1])
```

```python
import functools

import jax
import jax.numpy as jnp
from jax import lax
from jax.experimental import pallas as pl
from jax.experimental.pallas import tpu as pltpu
from jax.sharding import PartitionSpec as P

MESH = pl.DeviceIdType.MESH
EPS = 1e-6
LOG_BASE = 9.210340371976184
F32 = jnp.float32
BF16 = jnp.bfloat16
NT = (((1,), (1,)), ((), ()))
VMEM_LIMIT = 60 * 1024 * 1024


def mm(a, b):
    return jnp.dot(a, b, preferred_element_type=F32)


def rms(v, gain):
    inv = lax.rsqrt(jnp.mean(v * v, axis=-1, keepdims=True) + EPS)
    return (v * inv * gain).astype(BF16)


def attn_kernel(layer, x_ref, len_s, len_v, ag_ref, kg_ref, qg_ref, cache, w_dkv, w_qa, w_qb, w_uk, w_uv, w_o, part_ref, out_cache,
                c_v, dkv_v, qa_v, qb_v, uk_v, uv_v, o_v, qlow_s, ent_s, qs, qb16, sc_s, p_s, os, ho_s, wsem, csem, osem):
    rows, lat, rope, heads, qk = 32, 512, 64, 4, 192
    slots = c_v.shape[2]
    per = 4
    groups = rows // per
    width = 512
    qa_n = qa_v.shape[1] // width
    copies = []
    for n in range(qa_n):
        copies.append(pltpu.make_async_copy(w_qa.at[layer, :, pl.ds(n * width, width)], qa_v.at[:, pl.ds(n * width, width)], wsem.at[n]))
    copies.append(pltpu.make_async_copy(w_dkv.at[layer], dkv_v, wsem.at[qa_n]))
    copies.append(pltpu.make_async_copy(w_qb.at[layer], qb_v, wsem.at[qa_n + 1]))
    copies.append(pltpu.make_async_copy(w_uk.at[layer], uk_v, wsem.at[qa_n + 2]))
    copies.append(pltpu.make_async_copy(w_uv.at[layer], uv_v, wsem.at[qa_n + 3]))
    copies.append(pltpu.make_async_copy(w_o.at[layer], o_v, wsem.at[qa_n + 4]))

    def cache_in(g):
        return pltpu.make_async_copy(cache.at[pl.ds(g * per, per)], c_v.at[pl.ds(g * per, per)], csem.at[g])

    def cache_out(g):
        return pltpu.make_async_copy(c_v.at[pl.ds(g * per, per)], out_cache.at[pl.ds(g * per, per)], osem.at[g])

    for n in range(qa_n + 3):
        copies[n].start()

    xf = x_ref[...].astype(F32)
    h = rms(xf, ag_ref[layer:layer + 1, :])

    half = rope // 2
    lens_row = len_v[...].astype(F32)
    freq_t = jnp.exp(lax.broadcasted_iota(jnp.int32, (half, rows), 0).astype(F32) * (-LOG_BASE / half))
    ang_t = freq_t * jnp.broadcast_to(lens_row, (half, rows))
    cos_t, sin_t = jnp.cos(ang_t), jnp.sin(ang_t)
    cos_r, sin_r = cos_t.T, sin_t.T

    ssq = jnp.zeros((rows, 1), F32)
    for n in range(qa_n):
        copies[n].wait()
        if n == 0:
            for g in range(2):
                cache_in(g).start()
        part = mm(h, qa_v[:, n * width:(n + 1) * width])
        ssq = ssq + jnp.sum(part * part, axis=-1, keepdims=True)
        qlow_s[:, n * width:(n + 1) * width] = part
    for g in range(2, groups):
        cache_in(g).start()
    copies[qa_n].wait()
    kt = lax.dot_general(dkv_v[...], h, NT, preferred_element_type=F32)
    kl = kt[:lat]
    inv_k = lax.rsqrt(jnp.mean(kl * kl, axis=0, keepdims=True) + EPS)
    gain_t = jnp.broadcast_to(kg_ref[layer:layer + 1, :], (128, lat)).T[:, :rows]
    ent_s[0:lat, 0:rows] = (kl * inv_k * gain_t).astype(BF16).astype(F32)
    ka, kb = kt[lat:lat + half], kt[lat + half:]
    ent_s[lat:lat + half, 0:rows] = (ka * cos_t - kb * sin_t).astype(BF16).astype(F32)
    ent_s[lat + half:, 0:rows] = (kb * cos_t + ka * sin_t).astype(BF16).astype(F32)

    inv_q = lax.rsqrt(ssq / (qa_n * width) + EPS)
    copies[qa_n + 1].wait()
    q_low = (qlow_s[...] * inv_q * qg_ref[layer:layer + 1, :]).astype(BF16)
    q_full = mm(q_low, qb_v[...])
    copies[qa_n + 2].wait()
    for hd in range(heads):
        qh = q_full[:, hd * qk:(hd + 1) * qk]
        q_lat = mm(qh[:, :128].astype(BF16), uk_v[hd])
        for c in range(lat // 128):
            qs[c, pl.ds(hd, rows, stride=heads), :] = q_lat[:, c * 128:(c + 1) * 128]
        qa, qb = qh[:, 128:128 + half], qh[:, 128 + half:]
        rot = jnp.concatenate([qa * cos_r - qb * sin_r, qb * cos_r + qa * sin_r, jnp.zeros((rows, 128 - rope), F32)], axis=-1)
        qs[lat // 128, pl.ds(hd, rows, stride=heads), :] = rot
    for c in range(lat // 128 + 1):
        qb16[:, c * 128:(c + 1) * 128] = qs[c].astype(BF16)
    copies[qa_n + 3].start()
    copies[qa_n + 4].start()

    lane = lax.broadcasted_iota(jnp.int32, (1, slots), 1)
    lane_full = lax.broadcasted_iota(jnp.int32, (per * heads, slots), 1)
    row_of = lax.broadcasted_iota(jnp.int32, (per * heads, 1), 0) // heads
    row_w = lax.broadcasted_iota(jnp.int32, (per * heads, slots), 0) // heads
    row_l = lax.broadcasted_iota(jnp.int32, (per * heads, lat), 0) // heads
    scale = float(qk) ** -0.5

    def score_group(g):
        q16 = qb16[pl.ds(pl.multiple_of(g * 16, 16), 16), 0:lat + rope]
        ent = ent_s[...]
        acc = None
        for i in range(per):
            r = g * per + i
            n_r = len_s[r]
            col = jnp.broadcast_to(ent[:, i:i + 1], (lat + rope, slots)).astype(BF16)
            hit = jnp.broadcast_to(lane == n_r, (lat + rope, slots))
            new = jnp.where(hit, col, c_v[r])
            c_v[r] = new
            s_i = mm(q16, new) * scale
            s_i = jnp.where(lane_full <= n_r, s_i, -1e30)
            acc = s_i if acc is None else jnp.where(row_w == i, s_i, acc)
        ent_s[...] = pltpu.roll(ent, 128 - per, 1)
        sc_s[pl.ds(pl.multiple_of(g * 16, 16), 16), :] = acc

    def score_loop(g, c):
        cache_in(g).wait()
        score_group(g)
        cache_out(g).start()
        return c

    lax.fori_loop(0, groups, score_loop, 0)
    s = sc_s[...]
    e = jnp.exp(s - jnp.max(s, axis=-1, keepdims=True))
    p_s[...] = (e / jnp.sum(e, axis=-1, keepdims=True)).astype(BF16)

    def out_loop(g, c):
        p16 = p_s[pl.ds(pl.multiple_of(g * 16, 16), 16), :]
        acc = None
        for i in range(per):
            o_i = lax.dot_general(p16, c_v[g * per + i, 0:lat, :], NT, preferred_element_type=F32)
            acc = o_i if acc is None else jnp.where(row_l == i, o_i, acc)
        for c in range(lat // 128):
            os[c, pl.ds(pl.multiple_of(g * 16, 16), 16), :] = acc[:, c * 128:(c + 1) * 128]
        return c

    lax.fori_loop(0, groups, out_loop, 0)
    copies[qa_n + 3].wait()
    for hd in range(heads):
        o_lat = jnp.concatenate([os[c, pl.ds(hd, rows, stride=heads), :].astype(BF16) for c in range(lat // 128)], axis=-1)
        ho_s[:, hd * 128:(hd + 1) * 128] = mm(o_lat, uv_v[hd]).astype(BF16)
    copies[qa_n + 4].wait()
    ho = ho_s[...]
    for n in range(4):
        part_ref[:, n * 512:(n + 1) * 512] = mm(ho, o_v[:, n * 512:(n + 1) * 512])
    for g in range(groups):
        cache_out(g).wait()


def attn_call(layer, x, lengths, attn_gain, kv_gain, q_gain, cache_t, w_dkv_t, w_qa, w_qb, w_uk, w_uv, w_o):
    any_spec = pl.BlockSpec(memory_space=pl.ANY)
    vmem = pl.BlockSpec(memory_space=pltpu.VMEM)
    smem = pl.BlockSpec(memory_space=pltpu.SMEM)
    rows, width, slots = cache_t.shape
    heads = w_uk.shape[1]
    return pl.pallas_call(
        functools.partial(attn_kernel, layer),
        out_shape=(jax.ShapeDtypeStruct(x.shape, F32), jax.ShapeDtypeStruct(cache_t.shape, BF16)),
        in_specs=[vmem, smem, vmem, vmem, vmem, vmem] + [any_spec] * 7,
        out_specs=(vmem, any_spec),
        scratch_shapes=[
            pltpu.VMEM(cache_t.shape, BF16),
            pltpu.VMEM(w_dkv_t.shape[1:], BF16),
            pltpu.VMEM(w_qa.shape[1:], BF16),
            pltpu.VMEM(w_qb.shape[1:], BF16),
            pltpu.VMEM(w_uk.shape[1:], BF16),
            pltpu.VMEM(w_uv.shape[1:], BF16),
            pltpu.VMEM(w_o.shape[1:], BF16),
            pltpu.VMEM((rows, w_qa.shape[2]), F32),
            pltpu.VMEM((width, 128), F32),
            pltpu.VMEM((5, rows * heads, 128), F32),
            pltpu.VMEM((rows * heads, 640), BF16),
            pltpu.VMEM((rows * heads, slots), F32),
            pltpu.VMEM((rows * heads, slots), BF16),
            pltpu.VMEM((4, rows * heads, 128), F32),
            pltpu.VMEM((rows, heads * 128), BF16),
            pltpu.SemaphoreType.DMA((8,)),
            pltpu.SemaphoreType.DMA((8,)),
            pltpu.SemaphoreType.DMA((8,)),
        ],
        compiler_params=pltpu.CompilerParams(vmem_limit_bytes=VMEM_LIMIT),
        cost_estimate=pl.CostEstimate(flops=2_000_000_000, bytes_accessed=33_000_000, transcendentals=0),
        name=f"attn{layer}",
    )(x, lengths, lengths.reshape(1, rows), attn_gain, kv_gain, q_gain, cache_t, w_dkv_t, w_qa, w_qb, w_uk, w_uv, w_o)


def ffn_kernel(layer, n_tp, n_dp, part_ref, x_ref, fg_ref, w_gate, w_up, w_down, out_ref,
               g_v, u_v, d_v, rs_buf, xm_s, g_snd, g_buf, hid, f_snd, f_buf, x_snd,
               wsem, s_rs, r_rs, s_g, r_g, s_f, r_f, s_x, r_x):
    z = lax.axis_index("tp")
    d = lax.axis_index("dp")
    hid_w = g_v.shape[1]
    start = pl.multiple_of(d * hid_w, hid_w)
    half = hid_w // 2
    loads = []
    for c in range(2):
        loads.append(pltpu.make_async_copy(w_gate.at[layer, :, pl.ds(pl.multiple_of(start + c * half, 128), half)], g_v.at[:, pl.ds(c * half, half)], wsem.at[3 * c]))
        loads.append(pltpu.make_async_copy(w_up.at[layer, :, pl.ds(pl.multiple_of(start + c * half, 128), half)], u_v.at[:, pl.ds(c * half, half)], wsem.at[3 * c + 1]))
    for c in range(2):
        loads.append(pltpu.make_async_copy(w_down.at[layer, pl.ds(start + c * half, half), :], d_v.at[pl.ds(c * half, half), :], wsem.at[3 * c + 2]))
    for cp in loads:
        cp.start()

    tp_peers = [lax.rem(z + k, n_tp) for k in range(1, n_tp)]
    dp_peers = [lax.rem(d + k, n_dp) for k in range(1, n_dp)]
    barrier = pltpu.get_barrier_semaphore()
    for pz in tp_peers:
        pl.semaphore_signal(barrier, inc=1, device_id={"tp": pz}, device_id_type=MESH)
    for pd in dp_peers:
        pl.semaphore_signal(barrier, inc=1, device_id={"dp": pd}, device_id_type=MESH)
    pl.semaphore_wait(barrier, n_tp + n_dp - 2)

    def exchange(peers, axis, src_of, dst_of, ssem, rsem):
        cps = []
        for k, p in enumerate(peers):
            cps.append(pltpu.make_async_remote_copy(src_ref=src_of(k, p), dst_ref=dst_of(k), send_sem=ssem.at[k], recv_sem=rsem.at[k], device_id={axis: p}, device_id_type=MESH))
        return cps

    rs = exchange(tp_peers, "tp", lambda k, p: part_ref.at[p], lambda k: rs_buf.at[k], s_rs, r_rs)
    for cp in rs:
        cp.start()
    acc = x_ref[z].astype(F32)
    tot = part_ref[z]
    for k, cp in enumerate(rs):
        cp.wait_recv()
        tot = tot + rs_buf[k]
    xm = (acc + tot).astype(BF16).astype(F32)
    xm_s[...] = xm
    g = rms(xm, fg_ref[layer:layer + 1, :])
    g_snd[...] = g
    gx = exchange(dp_peers, "dp", lambda k, p: g_snd, lambda k: g_buf.at[k], s_g, r_g)
    for cp in gx:
        cp.start()
    for cp in gx:
        cp.wait_recv()
    full = jnp.concatenate([g.astype(F32)] + [g_buf[k].astype(F32) for k in range(n_dp - 1)], axis=0).astype(BF16)

    tile = 256
    for j in range(hid_w // tile):
        if j == 0:
            loads[0].wait()
            loads[1].wait()
        if (j + 1) * tile > half and j * tile <= half:
            loads[2].wait()
            loads[3].wait()
        gate = mm(full, g_v[:, j * tile:(j + 1) * tile])
        up = mm(full, u_v[:, j * tile:(j + 1) * tile])
        hid[:, j * tile:(j + 1) * tile] = (gate * jax.nn.sigmoid(gate) * up).astype(BF16)
    loads[4].wait()
    loads[5].wait()
    hv = hid[...]
    own = []
    for j in range(4):
        y = mm(hv, d_v[:, j * 512:(j + 1) * 512])
        for k in range(n_dp):
            f_snd[k, :, j * 512:(j + 1) * 512] = y[k * 8:(k + 1) * 8].astype(BF16)
    fx = []
    for k, p in enumerate(dp_peers):
        fx.append(pltpu.make_async_remote_copy(src_ref=f_snd.at[n_dp - 1 - k], dst_ref=f_buf.at[k], send_sem=s_f.at[k], recv_sem=r_f.at[k], device_id={"dp": p}, device_id_type=MESH))
    for cp in fx:
        cp.start()
    tot = f_snd[0].astype(F32)
    for k, cp in enumerate(fx):
        cp.wait_recv()
        tot = tot + f_buf[k].astype(F32)
    x_new = (xm_s[...] + tot).astype(BF16)
    x_snd[...] = x_new
    out_ref[z] = x_new
    xx = exchange(tp_peers, "tp", lambda k, p: x_snd, lambda k: out_ref.at[z], s_x, r_x)
    for cp in xx:
        cp.start()
    for cp in xx:
        cp.wait_recv()
    for cp in rs + gx + fx + xx:
        cp.wait_send()


def ffn_call(layer, n_tp, n_dp, part, x, ffn_gain, w_gate, w_up, w_down):
    any_spec = pl.BlockSpec(memory_space=pl.ANY)
    vmem = pl.BlockSpec(memory_space=pltpu.VMEM)
    rows, dim = x.shape
    own = rows // n_tp
    hid_w = w_gate.shape[2] // n_dp
    dma = pltpu.SemaphoreType.DMA
    out = pl.pallas_call(
        functools.partial(ffn_kernel, layer, n_tp, n_dp),
        out_shape=jax.ShapeDtypeStruct((n_tp, own, dim), BF16),
        in_specs=[vmem, vmem, vmem] + [any_spec] * 3,
        out_specs=vmem,
        scratch_shapes=[
            pltpu.VMEM((dim, hid_w), BF16),
            pltpu.VMEM((dim, hid_w), BF16),
            pltpu.VMEM((hid_w, dim), BF16),
            pltpu.VMEM((n_tp - 1, own, dim), F32),
            pltpu.VMEM((own, dim), F32),
            pltpu.VMEM((own, dim), BF16),
            pltpu.VMEM((n_dp - 1, own, dim), BF16),
            pltpu.VMEM((own * n_dp, hid_w), BF16),
            pltpu.VMEM((n_dp, own, dim), BF16),
            pltpu.VMEM((n_dp - 1, own, dim), BF16),
            pltpu.VMEM((own, dim), BF16),
            dma((6,)), dma((3,)), dma((3,)), dma((3,)), dma((3,)), dma((3,)), dma((3,)), dma((3,)), dma((3,)),
        ],
        compiler_params=pltpu.CompilerParams(vmem_limit_bytes=VMEM_LIMIT, collective_id=layer, has_side_effects=True),
        cost_estimate=pl.CostEstimate(flops=1_100_000_000, bytes_accessed=35_000_000, transcendentals=0),
        name=f"ffn{layer}",
    )(part.reshape(n_tp, own, dim), x.reshape(n_tp, own, dim), ffn_gain, w_gate, w_up, w_down)
    return out.reshape(rows, dim)


def solution(mesh):
    n_tp = mesh.shape["tp"]
    n_dp = mesh.shape["dp"]
    row_spec = P(("rep", "dp"), None)
    cache_spec = P(("rep", "dp"), None, None)
    in_specs = (row_spec, P(("rep", "dp")), cache_spec, cache_spec, P(), P(), P(), P(), P(), P(), P(None, None, "tp"), P(None, "tp", None, None), P(None, "tp", None, None), P(None, "tp", None), P(), P(), P())
    out_specs = (row_spec, cache_spec, cache_spec)

    def local_step(x, lengths, cache0, cache1, attn_gain, kv_gain, q_gain, ffn_gain, w_dkv, w_qa, w_qb, w_uk, w_uv, w_o, w_gate, w_up, w_down):
        w_dkv_t = jnp.swapaxes(w_dkv, 1, 2)
        new_caches = []
        for layer, cache in enumerate((cache0, cache1)):
            part, new_cache = attn_call(layer, x, lengths, attn_gain, kv_gain, q_gain, jnp.swapaxes(cache, 1, 2), w_dkv_t, w_qa, w_qb, w_uk, w_uv, w_o)
            x = ffn_call(layer, n_tp, n_dp, part, x, ffn_gain, w_gate, w_up, w_down)
            new_caches.append(jnp.swapaxes(new_cache, 1, 2))
        return x, new_caches[0], new_caches[1]

    return jax.shard_map(local_step, mesh=mesh, in_specs=in_specs, out_specs=out_specs, check_vma=False)
```

```python
import functools

import jax
import jax.numpy as jnp
from jax import lax
from jax.experimental import pallas as pl
from jax.experimental.pallas import tpu as pltpu
from jax.sharding import PartitionSpec as P

MESH = pl.DeviceIdType.MESH
EPS = 1e-6
LOG_BASE = 9.210340371976184
F32 = jnp.float32
BF16 = jnp.bfloat16
NT = (((1,), (1,)), ((), ()))
VMEM_LIMIT = 60 * 1024 * 1024


def mm(a, b):
    return jnp.dot(a, b, preferred_element_type=F32)


def rms(v, gain):
    inv = lax.rsqrt(jnp.mean(v * v, axis=-1, keepdims=True) + EPS)
    return (v * inv * gain).astype(BF16)


def attn_kernel(layer, x_ref, len_s, len_v, ag_ref, kg_ref, qg_ref, cache, w_dkv, w_qa, w_qb, w_uk, w_uv, w_o, part_ref, out_cache,
                c_v, c_new, dkv_v, qa_v, qb_v, uk_v, uv_v, o_v, qlow_s, ent_f, qs, qb16, sc_s, p_s, os, ho_s, wsem, csem, osem):
    rows, lat, rope, heads, qk = 32, 512, 64, 4, 192
    slots = c_v.shape[2]
    per = 4
    groups = rows // per
    width = 512
    qa_n = qa_v.shape[1] // width
    copies = []
    for n in range(qa_n):
        copies.append(pltpu.make_async_copy(w_qa.at[layer, :, pl.ds(n * width, width)], qa_v.at[:, pl.ds(n * width, width)], wsem.at[n]))
    copies.append(pltpu.make_async_copy(w_dkv.at[layer], dkv_v, wsem.at[qa_n]))
    copies.append(pltpu.make_async_copy(w_qb.at[layer], qb_v, wsem.at[qa_n + 1]))
    copies.append(pltpu.make_async_copy(w_uk.at[layer], uk_v, wsem.at[qa_n + 2]))
    copies.append(pltpu.make_async_copy(w_uv.at[layer], uv_v, wsem.at[qa_n + 3]))
    copies.append(pltpu.make_async_copy(w_o.at[layer], o_v, wsem.at[qa_n + 4]))

    def cache_in(g):
        return pltpu.make_async_copy(cache.at[pl.ds(g * per, per)], c_v.at[pl.ds(g * per, per)], csem.at[g])

    def cache_out(g):
        return pltpu.make_async_copy(c_new.at[pl.ds(g * per, per)], out_cache.at[pl.ds(g * per, per)], osem.at[g])

    for n in range(qa_n + 3):
        copies[n].start()

    xf = x_ref[...].astype(F32)
    h = rms(xf, ag_ref[layer:layer + 1, :])

    half = rope // 2
    lens_row = len_v[...].astype(F32)
    freq_t = jnp.exp(lax.broadcasted_iota(jnp.int32, (half, rows), 0).astype(F32) * (-LOG_BASE / half))
    ang_t = freq_t * jnp.broadcast_to(lens_row, (half, rows))
    cos_t, sin_t = jnp.cos(ang_t), jnp.sin(ang_t)
    cos_r, sin_r = cos_t.T, sin_t.T

    ssq = jnp.zeros((rows, 1), F32)
    for n in range(qa_n):
        copies[n].wait()
        if n == 0:
            for g in range(2):
                cache_in(g).start()
        part = mm(h, qa_v[:, n * width:(n + 1) * width])
        ssq = ssq + jnp.sum(part * part, axis=-1, keepdims=True)
        qlow_s[:, n * width:(n + 1) * width] = part
    for g in range(2, groups):
        cache_in(g).start()
    copies[qa_n].wait()
    cut = (lat + rope) // 2
    kt = jnp.concatenate([lax.dot_general(dkv_v[0:cut], h, NT, preferred_element_type=F32), lax.dot_general(dkv_v[cut:], h, NT, preferred_element_type=F32)], axis=0)
    kl = kt[:lat]
    inv_k = lax.rsqrt(jnp.mean(kl * kl, axis=0, keepdims=True) + EPS)
    gain_t = jnp.broadcast_to(kg_ref[layer:layer + 1, :], (128, lat)).T[:, :rows]
    ent_f[0:lat, 0:rows] = (kl * inv_k * gain_t).astype(BF16).astype(F32)
    ka, kb = kt[lat:lat + half], kt[lat + half:]
    ent_f[lat:lat + half, 0:rows] = (ka * cos_t - kb * sin_t).astype(BF16).astype(F32)
    ent_f[lat + half:, 0:rows] = (kb * cos_t + ka * sin_t).astype(BF16).astype(F32)

    inv_q = lax.rsqrt(ssq / (qa_n * width) + EPS)
    copies[qa_n + 1].wait()
    q_low = (qlow_s[...] * inv_q * qg_ref[layer:layer + 1, :]).astype(BF16)
    q_full = mm(q_low, qb_v[...])
    copies[qa_n + 2].wait()
    for hd in range(heads):
        qh = q_full[:, hd * qk:(hd + 1) * qk]
        q_lat = mm(qh[:, :128].astype(BF16), uk_v[hd])
        for c in range(lat // 128):
            qs[c, pl.ds(hd, rows, stride=heads), :] = q_lat[:, c * 128:(c + 1) * 128]
        qa, qb = qh[:, 128:128 + half], qh[:, 128 + half:]
        rot = jnp.concatenate([qa * cos_r - qb * sin_r, qb * cos_r + qa * sin_r, jnp.zeros((rows, 128 - rope), F32)], axis=-1)
        qs[lat // 128, pl.ds(hd, rows, stride=heads), :] = rot
    for c in range(lat // 128 + 1):
        qb16[:, c * 128:(c + 1) * 128] = qs[c].astype(BF16)
    copies[qa_n + 3].start()
    copies[qa_n + 4].start()

    lane = lax.broadcasted_iota(jnp.int32, (1, slots), 1)
    row_w = lax.broadcasted_iota(jnp.int32, (per * heads, slots), 0) // heads
    row_l = lax.broadcasted_iota(jnp.int32, (per * heads, lat), 0) // heads
    scale = float(qk) ** -0.5

    def insert(g):
        for i in range(per):
            r = g * per + i
            col = jnp.broadcast_to(ent_f[:, r:r + 1], (lat + rope, 128)).astype(BF16)
            hit = jnp.broadcast_to(lane == len_s[r], (lat + rope, slots))
            c_new[r] = jnp.where(hit, jnp.concatenate([col, col], axis=-1), c_v[r])
        cache_out(g).start()

    for g in range(groups):
        if g % 2 == 0:
            cache_in(g).wait()
            cache_in(g + 1).wait()
        q16 = qb16[g * 16:(g + 1) * 16, 0:lat + rope]
        acc = None
        for i in range(per):
            s_i = mm(q16, c_v[g * per + i])
            acc = s_i if acc is None else jnp.where(row_w == i, s_i, acc)
        sc_s[g * 16:(g + 1) * 16, :] = acc
        if g % 2 == 0:
            insert(g)
    pairs = rows * heads
    mine = lax.broadcasted_iota(jnp.int32, (pairs, rows), 0) // heads == lax.broadcasted_iota(jnp.int32, (pairs, rows), 1)
    ent = ent_f[:, 0:rows].astype(BF16)
    s_new = jnp.sum(jnp.where(mine, mm(qb16[:, 0:lat + rope], ent), 0.0), axis=-1, keepdims=True) * scale
    len_p = jnp.sum(jnp.where(mine, jnp.broadcast_to(lens_row, (pairs, rows)), 0.0), axis=-1, keepdims=True)
    lane_p = lax.broadcasted_iota(jnp.int32, (pairs, slots), 1).astype(F32)
    s = jnp.where(lane_p < len_p, sc_s[...] * scale, -1e30)
    top = jnp.maximum(jnp.max(s, axis=-1, keepdims=True), s_new)
    e = jnp.exp(s - top)
    e_new = jnp.exp(s_new - top)
    total = jnp.sum(e, axis=-1, keepdims=True) + e_new
    p_s[...] = jnp.where(lane_p < len_p, e / total, 0.0).astype(BF16)
    p_new = jnp.where(mine, jnp.broadcast_to(e_new / total, (pairs, rows)), 0.0).astype(BF16)
    o_new = lax.dot_general(p_new, ent[0:lat], NT, preferred_element_type=F32)
    for c in range(lat // 128):
        os[c] = o_new[:, c * 128:(c + 1) * 128]

    for g in range(groups):
        p16 = p_s[g * 16:(g + 1) * 16, :]
        acc = None
        for i in range(per):
            o_i = lax.dot_general(p16, c_v[g * per + i, 0:lat, :], NT, preferred_element_type=F32)
            acc = o_i if acc is None else jnp.where(row_l == i, o_i, acc)
        for c in range(lat // 128):
            os[c, g * 16:(g + 1) * 16, :] += acc[:, c * 128:(c + 1) * 128]
        if g % 2 == 1:
            insert(g)
    copies[qa_n + 3].wait()
    for hd in range(heads):
        o_lat = jnp.concatenate([os[c, pl.ds(hd, rows, stride=heads), :].astype(BF16) for c in range(lat // 128)], axis=-1)
        ho_s[:, hd * 128:(hd + 1) * 128] = mm(o_lat, uv_v[hd]).astype(BF16)
    copies[qa_n + 4].wait()
    ho = ho_s[...]
    for n in range(4):
        part_ref[:, n * 512:(n + 1) * 512] = mm(ho, o_v[:, n * 512:(n + 1) * 512])
    for g in range(groups):
        cache_out(g).wait()


def attn_call(layer, x, lengths, attn_gain, kv_gain, q_gain, cache_t, w_dkv_t, w_qa, w_qb, w_uk, w_uv, w_o):
    any_spec = pl.BlockSpec(memory_space=pl.ANY)
    vmem = pl.BlockSpec(memory_space=pltpu.VMEM)
    smem = pl.BlockSpec(memory_space=pltpu.SMEM)
    rows, width, slots = cache_t.shape
    heads = w_uk.shape[1]
    return pl.pallas_call(
        functools.partial(attn_kernel, layer),
        out_shape=(jax.ShapeDtypeStruct(x.shape, F32), jax.ShapeDtypeStruct(cache_t.shape, BF16)),
        in_specs=[vmem, smem, vmem, vmem, vmem, vmem] + [any_spec] * 7,
        out_specs=(vmem, any_spec),
        scratch_shapes=[
            pltpu.VMEM(cache_t.shape, BF16),
            pltpu.VMEM(cache_t.shape, BF16),
            pltpu.VMEM(w_dkv_t.shape[1:], BF16),
            pltpu.VMEM(w_qa.shape[1:], BF16),
            pltpu.VMEM(w_qb.shape[1:], BF16),
            pltpu.VMEM(w_uk.shape[1:], BF16),
            pltpu.VMEM(w_uv.shape[1:], BF16),
            pltpu.VMEM(w_o.shape[1:], BF16),
            pltpu.VMEM((rows, w_qa.shape[2]), F32),
            pltpu.VMEM((width, 128), F32),
            pltpu.VMEM((5, rows * heads, 128), F32),
            pltpu.VMEM((rows * heads, 640), BF16),
            pltpu.VMEM((rows * heads, slots), F32),
            pltpu.VMEM((rows * heads, slots), BF16),
            pltpu.VMEM((4, rows * heads, 128), F32),
            pltpu.VMEM((rows, heads * 128), BF16),
            pltpu.SemaphoreType.DMA((8,)),
            pltpu.SemaphoreType.DMA((8,)),
            pltpu.SemaphoreType.DMA((8,)),
        ],
        compiler_params=pltpu.CompilerParams(vmem_limit_bytes=VMEM_LIMIT),
        cost_estimate=pl.CostEstimate(flops=2_000_000_000, bytes_accessed=33_000_000, transcendentals=0),
        name=f"attn{layer}",
    )(x, lengths, lengths.reshape(1, rows), attn_gain, kv_gain, q_gain, cache_t, w_dkv_t, w_qa, w_qb, w_uk, w_uv, w_o)


def ffn_kernel(layer, n_tp, n_dp, part, x, gain, w_gate, w_up, w_down, out_ref,
               part_v, x_v, gain_v, g_v, u_v, d_v, rs_buf, xm_s, g_all, hid, f_snd, f_buf, x_snd,
               isem, wsem, s_rs, r_rs, s_g, r_g, s_f, r_f, s_x, r_x):
    z = lax.axis_index("tp")
    d = lax.axis_index("dp")
    tp_peers = [lax.rem(z + k, n_tp) for k in range(1, n_tp)]
    dp_peers = [lax.rem(d + k, n_dp) for k in range(1, n_dp)]
    barrier = pltpu.get_barrier_semaphore()
    for pz in tp_peers:
        pl.semaphore_signal(barrier, inc=1, device_id={"tp": pz}, device_id_type=MESH)
    for pd in dp_peers:
        pl.semaphore_signal(barrier, inc=1, device_id={"dp": pd}, device_id_type=MESH)

    ins = [pltpu.make_async_copy(part, part_v, isem.at[0]), pltpu.make_async_copy(x.at[z], x_v, isem.at[1]), pltpu.make_async_copy(gain, gain_v, isem.at[2])]
    for cp in ins:
        cp.start()
    hid_w = g_v.shape[1]
    start = pl.multiple_of(d * hid_w, hid_w)
    half = hid_w // 2
    loads = []
    for c in range(2):
        cols = pl.ds(pl.multiple_of(start + c * half, 128), half)
        loads.append(pltpu.make_async_copy(w_gate.at[layer, :, cols], g_v.at[:, pl.ds(c * half, half)], wsem.at[2 * c]))
        loads.append(pltpu.make_async_copy(w_up.at[layer, :, cols], u_v.at[:, pl.ds(c * half, half)], wsem.at[2 * c + 1]))
    for c in range(2):
        loads.append(pltpu.make_async_copy(w_down.at[layer, pl.ds(start + c * half, half), :], d_v.at[pl.ds(c * half, half), :], wsem.at[4 + c]))
    for cp in loads:
        cp.start()

    dim = x_v.shape[1]
    own = x_v.shape[0]
    chunks = 4
    wide = dim // chunks

    def send(axis, peer, src, dst, ssem, rsem, i):
        cp = pltpu.make_async_remote_copy(src_ref=src, dst_ref=dst, send_sem=ssem.at[i], recv_sem=rsem.at[i], device_id={axis: peer}, device_id_type=MESH)
        cp.start()
        return cp

    pl.semaphore_wait(barrier, n_tp + n_dp - 2)
    for cp in ins:
        cp.wait()
    rs, gx, fx, xx = [], [], [], []
    for c in range(chunks):
        cols = pl.ds(c * wide, wide)
        for k, p in enumerate(tp_peers):
            rs.append(send("tp", p, part_v.at[p, :, cols], rs_buf.at[k, :, cols], s_rs, r_rs, c * (n_tp - 1) + k))
    for c in range(chunks):
        cols = slice(c * wide, (c + 1) * wide)
        tot = part_v[z, :, cols]
        for k in range(n_tp - 1):
            rs[c * (n_tp - 1) + k].wait_recv()
            tot = tot + rs_buf[k, :, cols]
        xm = (x_v[:, cols].astype(F32) + tot).astype(BF16)
        xm_s[:, cols] = xm.astype(F32)
        g_all[0, :, cols] = xm
        for k, p in enumerate(dp_peers):
            gx.append(send("dp", p, g_all.at[0, :, pl.ds(c * wide, wide)], g_all.at[k + 1, :, pl.ds(c * wide, wide)], s_g, r_g, c * (n_dp - 1) + k))
    for cp in gx:
        cp.wait_recv()
    mids = jnp.concatenate([g_all[k].astype(F32) for k in range(n_dp)], axis=0)
    full = rms(mids, gain_v[layer:layer + 1, :])

    tile = 256
    for j in range(hid_w // tile):
        if j == 0:
            loads[0].wait()
            loads[1].wait()
        if (j + 1) * tile > half and j * tile <= half:
            loads[2].wait()
            loads[3].wait()
        gate = mm(full, g_v[:, j * tile:(j + 1) * tile])
        up = mm(full, u_v[:, j * tile:(j + 1) * tile])
        hid[:, j * tile:(j + 1) * tile] = (gate * jax.nn.sigmoid(gate) * up).astype(BF16)
    loads[4].wait()
    loads[5].wait()
    hv = hid[...]
    for c in range(chunks):
        y = mm(hv, d_v[:, c * wide:(c + 1) * wide])
        for b in range(n_dp):
            f_snd[b, :, c * wide:(c + 1) * wide] = y[b * own:(b + 1) * own].astype(BF16)
        cols = pl.ds(c * wide, wide)
        for k, p in enumerate(dp_peers):
            fx.append(send("dp", p, f_snd.at[n_dp - 1 - k, :, cols], f_buf.at[k, :, cols], s_f, r_f, c * (n_dp - 1) + k))
    for c in range(chunks):
        cols = slice(c * wide, (c + 1) * wide)
        tot = f_snd[0, :, cols].astype(F32)
        for k in range(n_dp - 1):
            fx[c * (n_dp - 1) + k].wait_recv()
            tot = tot + f_buf[k, :, cols].astype(F32)
        x_new = (xm_s[:, cols] + tot).astype(BF16)
        x_snd[:, cols] = x_new
        out_ref[z, :, cols] = x_new
        for k, p in enumerate(tp_peers):
            xx.append(send("tp", p, x_snd.at[:, pl.ds(c * wide, wide)], out_ref.at[z, :, pl.ds(c * wide, wide)], s_x, r_x, c * (n_tp - 1) + k))
    for cp in xx:
        cp.wait_recv()
    for cp in rs + gx + fx + xx:
        cp.wait_send()


def ffn_call(layer, n_tp, n_dp, part, x, ffn_gain, w_gate, w_up, w_down):
    any_spec = pl.BlockSpec(memory_space=pl.ANY)
    vmem = pl.BlockSpec(memory_space=pltpu.VMEM)
    rows, dim = x.shape
    own = rows // n_tp
    hid_w = w_gate.shape[2] // n_dp
    dma = pltpu.SemaphoreType.DMA
    sends = dma((4 * (n_tp - 1),))
    out = pl.pallas_call(
        functools.partial(ffn_kernel, layer, n_tp, n_dp),
        out_shape=jax.ShapeDtypeStruct((n_tp, own, dim), BF16),
        in_specs=[any_spec] * 6,
        out_specs=vmem,
        scratch_shapes=[
            pltpu.VMEM((n_tp, own, dim), F32),
            pltpu.VMEM((own, dim), BF16),
            pltpu.VMEM(ffn_gain.shape, F32),
            pltpu.VMEM((dim, hid_w), BF16),
            pltpu.VMEM((dim, hid_w), BF16),
            pltpu.VMEM((hid_w, dim), BF16),
            pltpu.VMEM((n_tp - 1, own, dim), F32),
            pltpu.VMEM((own, dim), F32),
            pltpu.VMEM((n_dp, own, dim), BF16),
            pltpu.VMEM((own * n_dp, hid_w), BF16),
            pltpu.VMEM((n_dp, own, dim), BF16),
            pltpu.VMEM((n_dp - 1, own, dim), BF16),
            pltpu.VMEM((own, dim), BF16),
            dma((3,)), dma((6,)), sends, sends, sends, sends, sends, sends, sends, sends,
        ],
        compiler_params=pltpu.CompilerParams(vmem_limit_bytes=VMEM_LIMIT, collective_id=layer, has_side_effects=True),
        cost_estimate=pl.CostEstimate(flops=1_100_000_000, bytes_accessed=35_000_000, transcendentals=0),
        name=f"ffn{layer}",
    )(part.reshape(n_tp, own, dim), x.reshape(n_tp, own, dim), ffn_gain, w_gate, w_up, w_down)
    return out.reshape(rows, dim)


def solution(mesh):
    n_tp = mesh.shape["tp"]
    n_dp = mesh.shape["dp"]
    row_spec = P(("rep", "dp"), None)
    cache_spec = P(("rep", "dp"), None, None)
    in_specs = (row_spec, P(("rep", "dp")), cache_spec, cache_spec, P(), P(), P(), P(), P(), P(), P(None, None, "tp"), P(None, "tp", None, None), P(None, "tp", None, None), P(None, "tp", None), P(), P(), P())
    out_specs = (row_spec, cache_spec, cache_spec)

    def local_step(x, lengths, cache0, cache1, attn_gain, kv_gain, q_gain, ffn_gain, w_dkv, w_qa, w_qb, w_uk, w_uv, w_o, w_gate, w_up, w_down):
        w_dkv_t = jnp.swapaxes(w_dkv, 1, 2)
        new_caches = []
        for layer, cache in enumerate((cache0, cache1)):
            part, new_cache = attn_call(layer, x, lengths, attn_gain, kv_gain, q_gain, jnp.swapaxes(cache, 1, 2), w_dkv_t, w_qa, w_qb, w_uk, w_uv, w_o)
            x = ffn_call(layer, n_tp, n_dp, part, x, ffn_gain, w_gate, w_up, w_down)
            new_caches.append(jnp.swapaxes(new_cache, 1, 2))
        return x, new_caches[0], new_caches[1]

    return jax.shard_map(local_step, mesh=mesh, in_specs=in_specs, out_specs=out_specs, check_vma=False)
```

```python
import functools

import jax
import jax.numpy as jnp
from jax import lax
from jax.experimental import pallas as pl
from jax.experimental.pallas import tpu as pltpu
from jax.sharding import PartitionSpec as P

MESH = pl.DeviceIdType.MESH
EPS = 1e-6
LOG_BASE = 9.210340371976184
F32 = jnp.float32
BF16 = jnp.bfloat16
NT = (((1,), (1,)), ((), ()))
VMEM_LIMIT = 60 * 1024 * 1024


def mm(a, b):
    return jnp.dot(a, b, preferred_element_type=F32)


def rms(v, gain):
    inv = lax.rsqrt(jnp.mean(v * v, axis=-1, keepdims=True) + EPS)
    return (v * inv * gain).astype(BF16)


def attn_kernel(layer, x_ref, len_s, len_v, ag_ref, kg_ref, qg_ref, cache, w_dkv, w_qa, w_qb, w_uk, w_uv, w_o, part_ref, out_cache,
                c_v, c_new, dkv_v, qa_v, qb_v, uk_v, uv_v, o_v, qlow_s, ent_f, qs, qb16, sc_s, p_s, os, ho_s, wsem, csem, osem):
    rows, lat, rope, heads, qk = 32, 512, 64, 4, 192
    slots = c_v.shape[2]
    per = 4
    groups = rows // per
    width = 512
    qa_n = qa_v.shape[1] // width
    copies = []
    for n in range(qa_n):
        copies.append(pltpu.make_async_copy(w_qa.at[layer, :, pl.ds(n * width, width)], qa_v.at[:, pl.ds(n * width, width)], wsem.at[n]))
    copies.append(pltpu.make_async_copy(w_dkv.at[layer], dkv_v, wsem.at[qa_n]))
    copies.append(pltpu.make_async_copy(w_qb.at[layer], qb_v, wsem.at[qa_n + 1]))
    copies.append(pltpu.make_async_copy(w_uk.at[layer], uk_v, wsem.at[qa_n + 2]))
    copies.append(pltpu.make_async_copy(w_uv.at[layer], uv_v, wsem.at[qa_n + 3]))
    copies.append(pltpu.make_async_copy(w_o.at[layer], o_v, wsem.at[qa_n + 4]))

    def cache_in(g):
        return pltpu.make_async_copy(cache.at[pl.ds(g * per, per)], c_v.at[pl.ds(g * per, per)], csem.at[g])

    def cache_out(g):
        return pltpu.make_async_copy(c_new.at[pl.ds(g * per, per)], out_cache.at[pl.ds(g * per, per)], osem.at[g])

    for n in range(qa_n + 3):
        copies[n].start()

    xf = x_ref[...].astype(F32)
    h = rms(xf, ag_ref[layer:layer + 1, :])

    half = rope // 2
    lens_row = len_v[...].astype(F32)
    freq_t = jnp.exp(lax.broadcasted_iota(jnp.int32, (half, rows), 0).astype(F32) * (-LOG_BASE / half))
    ang_t = freq_t * jnp.broadcast_to(lens_row, (half, rows))
    cos_t, sin_t = jnp.cos(ang_t), jnp.sin(ang_t)
    cos_r, sin_r = cos_t.T, sin_t.T

    ssq = jnp.zeros((rows, 1), F32)
    for n in range(qa_n):
        copies[n].wait()
        if n == 0:
            for g in range(2):
                cache_in(g).start()
        part = mm(h, qa_v[:, n * width:(n + 1) * width])
        ssq = ssq + jnp.sum(part * part, axis=-1, keepdims=True)
        qlow_s[:, n * width:(n + 1) * width] = part
    for g in range(2, groups):
        cache_in(g).start()
    copies[qa_n].wait()
    cut = (lat + rope) // 2
    kt = jnp.concatenate([lax.dot_general(dkv_v[0:cut], h, NT, preferred_element_type=F32), lax.dot_general(dkv_v[cut:], h, NT, preferred_element_type=F32)], axis=0)
    kl = kt[:lat]
    inv_k = lax.rsqrt(jnp.mean(kl * kl, axis=0, keepdims=True) + EPS)
    gain_t = jnp.broadcast_to(kg_ref[layer:layer + 1, :], (128, lat)).T[:, :rows]
    ent_f[0:lat, 0:rows] = (kl * inv_k * gain_t).astype(BF16).astype(F32)
    ka, kb = kt[lat:lat + half], kt[lat + half:]
    ent_f[lat:lat + half, 0:rows] = (ka * cos_t - kb * sin_t).astype(BF16).astype(F32)
    ent_f[lat + half:, 0:rows] = (kb * cos_t + ka * sin_t).astype(BF16).astype(F32)

    inv_q = lax.rsqrt(ssq / (qa_n * width) + EPS)
    copies[qa_n + 1].wait()
    q_low = (qlow_s[...] * inv_q * qg_ref[layer:layer + 1, :]).astype(BF16)
    q_full = mm(q_low, qb_v[...])
    copies[qa_n + 2].wait()
    for hd in range(heads):
        qh = q_full[:, hd * qk:(hd + 1) * qk]
        q_lat = mm(qh[:, :128].astype(BF16), uk_v[hd])
        for c in range(lat // 128):
            qs[c, pl.ds(hd, rows, stride=heads), :] = q_lat[:, c * 128:(c + 1) * 128]
        qa, qb = qh[:, 128:128 + half], qh[:, 128 + half:]
        rot = jnp.concatenate([qa * cos_r - qb * sin_r, qb * cos_r + qa * sin_r, jnp.zeros((rows, 128 - rope), F32)], axis=-1)
        qs[lat // 128, pl.ds(hd, rows, stride=heads), :] = rot
    for c in range(lat // 128 + 1):
        qb16[:, c * 128:(c + 1) * 128] = qs[c].astype(BF16)
    copies[qa_n + 3].start()
    copies[qa_n + 4].start()

    lane = lax.broadcasted_iota(jnp.int32, (1, slots), 1)
    row_w = lax.broadcasted_iota(jnp.int32, (per * heads, slots), 0) // heads
    row_l = lax.broadcasted_iota(jnp.int32, (per * heads, lat), 0) // heads
    scale = float(qk) ** -0.5

    def insert(g):
        for i in range(per):
            r = g * per + i
            col = jnp.broadcast_to(ent_f[:, r:r + 1], (lat + rope, 128)).astype(BF16)
            hit = jnp.broadcast_to(lane == len_s[r], (lat + rope, slots))
            c_new[r] = jnp.where(hit, jnp.concatenate([col, col], axis=-1), c_v[r])
        cache_out(g).start()

    for g in range(groups):
        if g % 2 == 0:
            cache_in(g).wait()
            cache_in(g + 1).wait()
        q16 = qb16[g * 16:(g + 1) * 16, 0:lat + rope]
        acc = None
        for i in range(per):
            s_i = mm(q16, c_v[g * per + i])
            acc = s_i if acc is None else jnp.where(row_w == i, s_i, acc)
        sc_s[g * 16:(g + 1) * 16, :] = acc
        if g % 2 == 0:
            insert(g)
    pairs = rows * heads
    mine = lax.broadcasted_iota(jnp.int32, (pairs, rows), 0) // heads == lax.broadcasted_iota(jnp.int32, (pairs, rows), 1)
    ent = ent_f[:, 0:rows].astype(BF16)
    s_new = jnp.sum(jnp.where(mine, mm(qb16[:, 0:lat + rope], ent), 0.0), axis=-1, keepdims=True) * scale
    len_p = jnp.sum(jnp.where(mine, jnp.broadcast_to(lens_row, (pairs, rows)), 0.0), axis=-1, keepdims=True)
    lane_p = lax.broadcasted_iota(jnp.int32, (pairs, slots), 1).astype(F32)
    s = jnp.where(lane_p < len_p, sc_s[...] * scale, -1e30)
    top = jnp.maximum(jnp.max(s, axis=-1, keepdims=True), s_new)
    e = jnp.exp(s - top)
    e_new = jnp.exp(s_new - top)
    total = jnp.sum(e, axis=-1, keepdims=True) + e_new
    p_s[...] = jnp.where(lane_p < len_p, e / total, 0.0).astype(BF16)
    p_new = jnp.where(mine, jnp.broadcast_to(e_new / total, (pairs, rows)), 0.0).astype(BF16)
    o_new = lax.dot_general(p_new, ent[0:lat], NT, preferred_element_type=F32)
    for c in range(lat // 128):
        os[c] = o_new[:, c * 128:(c + 1) * 128]

    for g in range(groups):
        p16 = p_s[g * 16:(g + 1) * 16, :]
        acc = None
        for i in range(per):
            o_i = lax.dot_general(p16, c_v[g * per + i, 0:lat, :], NT, preferred_element_type=F32)
            acc = o_i if acc is None else jnp.where(row_l == i, o_i, acc)
        for c in range(lat // 128):
            os[c, g * 16:(g + 1) * 16, :] += acc[:, c * 128:(c + 1) * 128]
        if g % 2 == 1:
            insert(g)
    copies[qa_n + 3].wait()
    for hd in range(heads):
        o_lat = jnp.concatenate([os[c, pl.ds(hd, rows, stride=heads), :].astype(BF16) for c in range(lat // 128)], axis=-1)
        ho_s[:, hd * 128:(hd + 1) * 128] = mm(o_lat, uv_v[hd]).astype(BF16)
    copies[qa_n + 4].wait()
    ho = ho_s[...]
    for n in range(4):
        part_ref[:, n * 512:(n + 1) * 512] = mm(ho, o_v[:, n * 512:(n + 1) * 512])
    for g in range(groups):
        cache_out(g).wait()


def attn_call(layer, x, lengths, attn_gain, kv_gain, q_gain, cache_t, w_dkv_t, w_qa, w_qb, w_uk, w_uv, w_o):
    any_spec = pl.BlockSpec(memory_space=pl.ANY)
    vmem = pl.BlockSpec(memory_space=pltpu.VMEM)
    smem = pl.BlockSpec(memory_space=pltpu.SMEM)
    rows, width, slots = cache_t.shape
    heads = w_uk.shape[1]
    return pl.pallas_call(
        functools.partial(attn_kernel, layer),
        out_shape=(jax.ShapeDtypeStruct(x.shape, F32), jax.ShapeDtypeStruct(cache_t.shape, BF16)),
        in_specs=[vmem, smem, vmem, vmem, vmem, vmem] + [any_spec] * 7,
        out_specs=(vmem, any_spec),
        scratch_shapes=[
            pltpu.VMEM(cache_t.shape, BF16),
            pltpu.VMEM(cache_t.shape, BF16),
            pltpu.VMEM(w_dkv_t.shape[1:], BF16),
            pltpu.VMEM(w_qa.shape[1:], BF16),
            pltpu.VMEM(w_qb.shape[1:], BF16),
            pltpu.VMEM(w_uk.shape[1:], BF16),
            pltpu.VMEM(w_uv.shape[1:], BF16),
            pltpu.VMEM(w_o.shape[1:], BF16),
            pltpu.VMEM((rows, w_qa.shape[2]), F32),
            pltpu.VMEM((width, 128), F32),
            pltpu.VMEM((5, rows * heads, 128), F32),
            pltpu.VMEM((rows * heads, 640), BF16),
            pltpu.VMEM((rows * heads, slots), F32),
            pltpu.VMEM((rows * heads, slots), BF16),
            pltpu.VMEM((4, rows * heads, 128), F32),
            pltpu.VMEM((rows, heads * 128), BF16),
            pltpu.SemaphoreType.DMA((8,)),
            pltpu.SemaphoreType.DMA((8,)),
            pltpu.SemaphoreType.DMA((8,)),
        ],
        compiler_params=pltpu.CompilerParams(vmem_limit_bytes=VMEM_LIMIT),
        cost_estimate=pl.CostEstimate(flops=2_000_000_000, bytes_accessed=33_000_000, transcendentals=0),
        name=f"attn{layer}",
    )(x, lengths, lengths.reshape(1, rows), attn_gain, kv_gain, q_gain, cache_t, w_dkv_t, w_qa, w_qb, w_uk, w_uv, w_o)


def ffn_kernel(layer, n_tp, n_dp, part, x, gain, w_gate, w_up, w_down, out_ref,
               part_v, x_v, gain_v, g_v, u_v, d_v, rs_buf, xm_s, g_all, hid, f_snd, f_buf, x_snd,
               isem, wsem, s_rs, r_rs, s_g, r_g, s_f, r_f, s_x, r_x):
    z = lax.axis_index("tp")
    d = lax.axis_index("dp")
    tp_peers = [lax.rem(z + k, n_tp) for k in range(1, n_tp)]
    dp_peers = [lax.rem(d + k, n_dp) for k in range(1, n_dp)]
    barrier = pltpu.get_barrier_semaphore()
    for pz in tp_peers:
        pl.semaphore_signal(barrier, inc=1, device_id={"tp": pz}, device_id_type=MESH)
    for pd in dp_peers:
        pl.semaphore_signal(barrier, inc=1, device_id={"dp": pd}, device_id_type=MESH)

    ins = [pltpu.make_async_copy(part, part_v, isem.at[0]), pltpu.make_async_copy(x.at[z], x_v, isem.at[1]), pltpu.make_async_copy(gain, gain_v, isem.at[2])]
    for cp in ins:
        cp.start()
    hid_w = g_v.shape[1]
    start = pl.multiple_of(d * hid_w, hid_w)
    quarter = g_v.shape[0] // 4
    wide_loads, down_loads = [], []
    for c in range(4):
        rows = pl.ds(c * quarter, quarter)
        wide_loads.append(pltpu.make_async_copy(w_gate.at[layer, rows, pl.ds(start, hid_w)], g_v.at[rows, :], wsem.at[c]))
        wide_loads.append(pltpu.make_async_copy(w_up.at[layer, rows, pl.ds(start, hid_w)], u_v.at[rows, :], wsem.at[4 + c]))
    for c in range(4):
        rows = hid_w // 4
        down_loads.append(pltpu.make_async_copy(w_down.at[layer, pl.ds(start + c * rows, rows), :], d_v.at[pl.ds(c * rows, rows), :], wsem.at[8 + c]))
    wide_loads[0].start()

    dim = x_v.shape[1]
    own = x_v.shape[0]
    chunks = 4
    wide = dim // chunks

    def send(axis, peer, src, dst, ssem, rsem, i):
        cp = pltpu.make_async_remote_copy(src_ref=src, dst_ref=dst, send_sem=ssem.at[i], recv_sem=rsem.at[i], device_id={axis: peer}, device_id_type=MESH)
        cp.start()
        return cp

    pl.semaphore_wait(barrier, n_tp + n_dp - 2)
    for cp in ins:
        cp.wait()
    rs, gx, fx, xx = [], [], [], []
    for c in range(chunks):
        cols = pl.ds(c * wide, wide)
        for k, p in enumerate(tp_peers):
            rs.append(send("tp", p, part_v.at[p, :, cols], rs_buf.at[k, :, cols], s_rs, r_rs, c * (n_tp - 1) + k))
    for cp in wide_loads[1:5]:
        cp.start()
    for c in range(chunks):
        cols = slice(c * wide, (c + 1) * wide)
        tot = part_v[z, :, cols]
        for k in range(n_tp - 1):
            rs[c * (n_tp - 1) + k].wait_recv()
            tot = tot + rs_buf[k, :, cols]
        xm = (x_v[:, cols].astype(F32) + tot).astype(BF16)
        xm_s[:, cols] = xm.astype(F32)
        g_all[0, :, cols] = xm
        for k, p in enumerate(dp_peers):
            gx.append(send("dp", p, g_all.at[0, :, pl.ds(c * wide, wide)], g_all.at[k + 1, :, pl.ds(c * wide, wide)], s_g, r_g, c * (n_dp - 1) + k))
        if c < 3:
            wide_loads[5 + c].start()
    for cp in down_loads:
        cp.start()
    for cp in gx:
        cp.wait_recv()
    mids = jnp.concatenate([g_all[k].astype(F32) for k in range(n_dp)], axis=0)
    full = rms(mids, gain_v[layer:layer + 1, :])

    for cp in wide_loads:
        cp.wait()
    tile = 256
    for j in range(hid_w // tile):
        gate = mm(full, g_v[:, j * tile:(j + 1) * tile])
        up = mm(full, u_v[:, j * tile:(j + 1) * tile])
        hid[:, j * tile:(j + 1) * tile] = (gate * jax.nn.sigmoid(gate) * up).astype(BF16)
    for cp in down_loads:
        cp.wait()
    hv = hid[...]
    for c in range(chunks):
        y = mm(hv, d_v[:, c * wide:(c + 1) * wide])
        for b in range(n_dp):
            f_snd[b, :, c * wide:(c + 1) * wide] = y[b * own:(b + 1) * own].astype(BF16)
        cols = pl.ds(c * wide, wide)
        for k, p in enumerate(dp_peers):
            fx.append(send("dp", p, f_snd.at[n_dp - 1 - k, :, cols], f_buf.at[k, :, cols], s_f, r_f, c * (n_dp - 1) + k))
    for c in range(chunks):
        cols = slice(c * wide, (c + 1) * wide)
        tot = f_snd[0, :, cols].astype(F32)
        for k in range(n_dp - 1):
            fx[c * (n_dp - 1) + k].wait_recv()
            tot = tot + f_buf[k, :, cols].astype(F32)
        x_new = (xm_s[:, cols] + tot).astype(BF16)
        x_snd[:, cols] = x_new
        out_ref[z, :, cols] = x_new
        for k, p in enumerate(tp_peers):
            xx.append(send("tp", p, x_snd.at[:, pl.ds(c * wide, wide)], out_ref.at[z, :, pl.ds(c * wide, wide)], s_x, r_x, c * (n_tp - 1) + k))
    for cp in xx:
        cp.wait_recv()
    for cp in rs + gx + fx + xx:
        cp.wait_send()


def ffn_call(layer, n_tp, n_dp, part, x, ffn_gain, w_gate, w_up, w_down):
    any_spec = pl.BlockSpec(memory_space=pl.ANY)
    vmem = pl.BlockSpec(memory_space=pltpu.VMEM)
    rows, dim = x.shape
    own = rows // n_tp
    hid_w = w_gate.shape[2] // n_dp
    dma = pltpu.SemaphoreType.DMA
    sends = dma((4 * (n_tp - 1),))
    out = pl.pallas_call(
        functools.partial(ffn_kernel, layer, n_tp, n_dp),
        out_shape=jax.ShapeDtypeStruct((n_tp, own, dim), BF16),
        in_specs=[any_spec] * 6,
        out_specs=vmem,
        scratch_shapes=[
            pltpu.VMEM((n_tp, own, dim), F32),
            pltpu.VMEM((own, dim), BF16),
            pltpu.VMEM(ffn_gain.shape, F32),
            pltpu.VMEM((dim, hid_w), BF16),
            pltpu.VMEM((dim, hid_w), BF16),
            pltpu.VMEM((hid_w, dim), BF16),
            pltpu.VMEM((n_tp - 1, own, dim), F32),
            pltpu.VMEM((own, dim), F32),
            pltpu.VMEM((n_dp, own, dim), BF16),
            pltpu.VMEM((own * n_dp, hid_w), BF16),
            pltpu.VMEM((n_dp, own, dim), BF16),
            pltpu.VMEM((n_dp - 1, own, dim), BF16),
            pltpu.VMEM((own, dim), BF16),
            dma((3,)), dma((12,)), sends, sends, sends, sends, sends, sends, sends, sends,
        ],
        compiler_params=pltpu.CompilerParams(vmem_limit_bytes=VMEM_LIMIT, collective_id=layer, has_side_effects=True),
        cost_estimate=pl.CostEstimate(flops=1_100_000_000, bytes_accessed=35_000_000, transcendentals=0),
        name=f"ffn{layer}",
    )(part.reshape(n_tp, own, dim), x.reshape(n_tp, own, dim), ffn_gain, w_gate, w_up, w_down)
    return out.reshape(rows, dim)


def solution(mesh):
    n_tp = mesh.shape["tp"]
    n_dp = mesh.shape["dp"]
    row_spec = P(("rep", "dp"), None)
    cache_spec = P(("rep", "dp"), None, None)
    in_specs = (row_spec, P(("rep", "dp")), cache_spec, cache_spec, P(), P(), P(), P(), P(), P(), P(None, None, "tp"), P(None, "tp", None, None), P(None, "tp", None, None), P(None, "tp", None), P(), P(), P())
    out_specs = (row_spec, cache_spec, cache_spec)

    def local_step(x, lengths, cache0, cache1, attn_gain, kv_gain, q_gain, ffn_gain, w_dkv, w_qa, w_qb, w_uk, w_uv, w_o, w_gate, w_up, w_down):
        w_dkv_t = jnp.swapaxes(w_dkv, 1, 2)
        new_caches = []
        for layer, cache in enumerate((cache0, cache1)):
            part, new_cache = attn_call(layer, x, lengths, attn_gain, kv_gain, q_gain, jnp.swapaxes(cache, 1, 2), w_dkv_t, w_qa, w_qb, w_uk, w_uv, w_o)
            x = ffn_call(layer, n_tp, n_dp, part, x, ffn_gain, w_gate, w_up, w_down)
            new_caches.append(jnp.swapaxes(new_cache, 1, 2))
        return x, new_caches[0], new_caches[1]

    return jax.shard_map(local_step, mesh=mesh, in_specs=in_specs, out_specs=out_specs, check_vma=False)
```

```python
import functools

import jax
import jax.numpy as jnp
from jax import lax
from jax.experimental import pallas as pl
from jax.experimental.pallas import tpu as pltpu
from jax.sharding import PartitionSpec as P

MESH = pl.DeviceIdType.MESH
EPS = 1e-6
LOG_BASE = 9.210340371976184
F32 = jnp.float32
BF16 = jnp.bfloat16
NT = (((1,), (1,)), ((), ()))
VMEM_LIMIT = 60 * 1024 * 1024


def mm(a, b):
    return jnp.dot(a, b, preferred_element_type=F32)


def rms(v, gain):
    inv = lax.rsqrt(jnp.mean(v * v, axis=-1, keepdims=True) + EPS)
    return (v * inv * gain).astype(BF16)


def attn_kernel(layer, x_ref, len_s, len_v, ag_ref, kg_ref, qg_ref, cache, w_dkv, w_qa, w_qb, w_uk, w_uv, w_o, part_ref, out_cache,
                c_v, c_new, dkv_v, qa_v, qb_v, uk_v, uv_v, o_v, qlow_s, ent_f, qs, qb16, sc_s, p_s, os, ho_s, wsem, csem, osem):
    rows, lat, rope, heads, qk = 32, 512, 64, 4, 192
    slots = c_v.shape[2]
    per = 4
    groups = rows // per
    width = 512
    qa_n = qa_v.shape[1] // width
    copies = []
    for n in range(qa_n):
        copies.append(pltpu.make_async_copy(w_qa.at[layer, :, pl.ds(n * width, width)], qa_v.at[:, pl.ds(n * width, width)], wsem.at[n]))
    for i, (src, dst) in enumerate(((w_dkv, dkv_v), (w_qb, qb_v), (w_uk, uk_v), (w_uv, uv_v), (w_o, o_v))):
        copies.append(pltpu.make_async_copy(src.at[layer], dst, wsem.at[qa_n + i]))

    def cache_in(g):
        return pltpu.make_async_copy(cache.at[pl.ds(g * per, per)], c_v.at[pl.ds(g * per, per)], csem.at[g])

    def cache_out(g):
        return pltpu.make_async_copy(c_new.at[pl.ds(g * per, per)], out_cache.at[pl.ds(g * per, per)], osem.at[g])

    for cp in [copies[qa_n]] + copies[:qa_n] + copies[qa_n + 1:qa_n + 3]:
        cp.start()
    for g in range(groups):
        cache_in(g).start()
    copies[qa_n + 3].start()
    copies[qa_n + 4].start()

    xf = x_ref[...].astype(F32)
    h = rms(xf, ag_ref[layer:layer + 1, :])

    half = rope // 2
    lens_row = len_v[...].astype(F32)
    freq_t = jnp.exp(lax.broadcasted_iota(jnp.int32, (half, rows), 0).astype(F32) * (-LOG_BASE / half))
    ang_t = freq_t * jnp.broadcast_to(lens_row, (half, rows))
    cos_t, sin_t = jnp.cos(ang_t), jnp.sin(ang_t)
    cos_r, sin_r = cos_t.T, sin_t.T

    copies[qa_n].wait()
    cut = (lat + rope) // 2
    kt = jnp.concatenate([lax.dot_general(dkv_v[0:cut], h, NT, preferred_element_type=F32), lax.dot_general(dkv_v[cut:], h, NT, preferred_element_type=F32)], axis=0)
    kl = kt[:lat]
    inv_k = lax.rsqrt(jnp.mean(kl * kl, axis=0, keepdims=True) + EPS)
    gain_t = jnp.broadcast_to(kg_ref[layer:layer + 1, :], (128, lat)).T[:, :rows]
    ent_f[0:lat, 0:rows] = (kl * inv_k * gain_t).astype(BF16).astype(F32)
    ka, kb = kt[lat:lat + half], kt[lat + half:]
    ent_f[lat:lat + half, 0:rows] = (ka * cos_t - kb * sin_t).astype(BF16).astype(F32)
    ent_f[lat + half:, 0:rows] = (kb * cos_t + ka * sin_t).astype(BF16).astype(F32)

    ssq = jnp.zeros((rows, 1), F32)
    for n in range(qa_n):
        copies[n].wait()
        part = mm(h, qa_v[:, n * width:(n + 1) * width])
        ssq = ssq + jnp.sum(part * part, axis=-1, keepdims=True)
        qlow_s[:, n * width:(n + 1) * width] = part
    inv_q = lax.rsqrt(ssq / (qa_n * width) + EPS)
    copies[qa_n + 1].wait()
    q_low = (qlow_s[...] * inv_q * qg_ref[layer:layer + 1, :]).astype(BF16)
    q_full = mm(q_low, qb_v[...])
    copies[qa_n + 2].wait()
    for hd in range(heads):
        qh = q_full[:, hd * qk:(hd + 1) * qk]
        q_lat = mm(qh[:, :128].astype(BF16), uk_v[hd])
        for c in range(lat // 128):
            qs[c, pl.ds(hd, rows, stride=heads), :] = q_lat[:, c * 128:(c + 1) * 128]
        qa, qb = qh[:, 128:128 + half], qh[:, 128 + half:]
        rot = jnp.concatenate([qa * cos_r - qb * sin_r, qb * cos_r + qa * sin_r, jnp.zeros((rows, 128 - rope), F32)], axis=-1)
        qs[lat // 128, pl.ds(hd, rows, stride=heads), :] = rot
    for c in range(lat // 128 + 1):
        qb16[:, c * 128:(c + 1) * 128] = qs[c].astype(BF16)

    lane = lax.broadcasted_iota(jnp.int32, (1, slots), 1)
    row_w = lax.broadcasted_iota(jnp.int32, (per * heads, slots), 0) // heads
    row_l = lax.broadcasted_iota(jnp.int32, (per * heads, lat), 0) // heads
    scale = float(qk) ** -0.5

    def insert(g):
        for i in range(per):
            r = g * per + i
            col = jnp.broadcast_to(ent_f[:, r:r + 1], (lat + rope, 128)).astype(BF16)
            hit = jnp.broadcast_to(lane == len_s[r], (lat + rope, slots))
            c_new[r] = jnp.where(hit, jnp.concatenate([col, col], axis=-1), c_v[r])
        cache_out(g).start()

    for g in range(groups):
        if g % 2 == 0:
            cache_in(g).wait()
            cache_in(g + 1).wait()
        q16 = qb16[g * 16:(g + 1) * 16, 0:lat + rope]
        acc = None
        for i in range(per):
            s_i = mm(q16, c_v[g * per + i])
            acc = s_i if acc is None else jnp.where(row_w == i, s_i, acc)
        sc_s[g * 16:(g + 1) * 16, :] = acc
        insert(g)
    pairs = rows * heads
    mine = lax.broadcasted_iota(jnp.int32, (pairs, rows), 0) // heads == lax.broadcasted_iota(jnp.int32, (pairs, rows), 1)
    ent = ent_f[:, 0:rows].astype(BF16)
    s_new = jnp.sum(jnp.where(mine, mm(qb16[:, 0:lat + rope], ent), 0.0), axis=-1, keepdims=True) * scale
    len_p = jnp.sum(jnp.where(mine, jnp.broadcast_to(lens_row, (pairs, rows)), 0.0), axis=-1, keepdims=True)
    lane_p = lax.broadcasted_iota(jnp.int32, (pairs, slots), 1).astype(F32)
    s = jnp.where(lane_p < len_p, sc_s[...] * scale, -1e30)
    top = jnp.maximum(jnp.max(s, axis=-1, keepdims=True), s_new)
    e = jnp.exp(s - top)
    e_new = jnp.exp(s_new - top)
    total = jnp.sum(e, axis=-1, keepdims=True) + e_new
    p_s[...] = jnp.where(lane_p < len_p, e / total, 0.0).astype(BF16)
    p_new = jnp.where(mine, jnp.broadcast_to(e_new / total, (pairs, rows)), 0.0).astype(BF16)
    o_new = lax.dot_general(p_new, ent[0:lat], NT, preferred_element_type=F32)
    for c in range(lat // 128):
        os[c] = o_new[:, c * 128:(c + 1) * 128]

    for g in range(groups):
        p16 = p_s[g * 16:(g + 1) * 16, :]
        acc = None
        for i in range(per):
            o_i = lax.dot_general(p16, c_v[g * per + i, 0:lat, :], NT, preferred_element_type=F32)
            acc = o_i if acc is None else jnp.where(row_l == i, o_i, acc)
        for c in range(lat // 128):
            os[c, g * 16:(g + 1) * 16, :] += acc[:, c * 128:(c + 1) * 128]
    copies[qa_n + 3].wait()
    for hd in range(heads):
        o_lat = jnp.concatenate([os[c, pl.ds(hd, rows, stride=heads), :].astype(BF16) for c in range(lat // 128)], axis=-1)
        ho_s[:, hd * 128:(hd + 1) * 128] = mm(o_lat, uv_v[hd]).astype(BF16)
    copies[qa_n + 4].wait()
    ho = ho_s[...]
    for n in range(4):
        part_ref[:, n * 512:(n + 1) * 512] = mm(ho, o_v[:, n * 512:(n + 1) * 512])
    for g in range(groups):
        cache_out(g).wait()


def attn_call(layer, x, lengths, attn_gain, kv_gain, q_gain, cache_t, w_dkv_t, w_qa, w_qb, w_uk, w_uv, w_o):
    any_spec = pl.BlockSpec(memory_space=pl.ANY)
    vmem = pl.BlockSpec(memory_space=pltpu.VMEM)
    smem = pl.BlockSpec(memory_space=pltpu.SMEM)
    rows, width, slots = cache_t.shape
    heads = w_uk.shape[1]
    return pl.pallas_call(
        functools.partial(attn_kernel, layer),
        out_shape=(jax.ShapeDtypeStruct(x.shape, F32), jax.ShapeDtypeStruct(cache_t.shape, BF16)),
        in_specs=[vmem, smem, vmem, vmem, vmem, vmem] + [any_spec] * 7,
        out_specs=(vmem, any_spec),
        scratch_shapes=[
            pltpu.VMEM(cache_t.shape, BF16),
            pltpu.VMEM(cache_t.shape, BF16),
            pltpu.VMEM(w_dkv_t.shape[1:], BF16),
            pltpu.VMEM(w_qa.shape[1:], BF16),
            pltpu.VMEM(w_qb.shape[1:], BF16),
            pltpu.VMEM(w_uk.shape[1:], BF16),
            pltpu.VMEM(w_uv.shape[1:], BF16),
            pltpu.VMEM(w_o.shape[1:], BF16),
            pltpu.VMEM((rows, w_qa.shape[2]), F32),
            pltpu.VMEM((width, 128), F32),
            pltpu.VMEM((5, rows * heads, 128), F32),
            pltpu.VMEM((rows * heads, 640), BF16),
            pltpu.VMEM((rows * heads, slots), F32),
            pltpu.VMEM((rows * heads, slots), BF16),
            pltpu.VMEM((4, rows * heads, 128), F32),
            pltpu.VMEM((rows, heads * 128), BF16),
            pltpu.SemaphoreType.DMA((8,)),
            pltpu.SemaphoreType.DMA((8,)),
            pltpu.SemaphoreType.DMA((8,)),
        ],
        compiler_params=pltpu.CompilerParams(vmem_limit_bytes=VMEM_LIMIT),
        cost_estimate=pl.CostEstimate(flops=2_000_000_000, bytes_accessed=33_000_000, transcendentals=0),
        name=f"attn{layer}",
    )(x, lengths, lengths.reshape(1, rows), attn_gain, kv_gain, q_gain, cache_t, w_dkv_t, w_qa, w_qb, w_uk, w_uv, w_o)


def ffn_kernel(layer, n_tp, n_dp, part, x, gain, w_gate, w_up, w_down, out_ref,
               part_v, x_v, gain_v, g_v, u_v, d_v, rs_buf, xm_s, g_all, hid, f_snd, f_buf, x_snd,
               isem, wsem, s_rs, r_rs, s_g, r_g, s_f, r_f, s_x, r_x):
    z = lax.axis_index("tp")
    d = lax.axis_index("dp")
    tp_peers = [lax.rem(z + k, n_tp) for k in range(1, n_tp)]
    dp_peers = [lax.rem(d + k, n_dp) for k in range(1, n_dp)]
    barrier = pltpu.get_barrier_semaphore()
    for pz in tp_peers:
        pl.semaphore_signal(barrier, inc=1, device_id={"tp": pz}, device_id_type=MESH)
    for pd in dp_peers:
        pl.semaphore_signal(barrier, inc=1, device_id={"dp": pd}, device_id_type=MESH)

    ins = [pltpu.make_async_copy(part, part_v, isem.at[0]), pltpu.make_async_copy(x.at[z], x_v, isem.at[1]), pltpu.make_async_copy(gain, gain_v, isem.at[2])]
    for cp in ins:
        cp.start()
    hid_w = g_v.shape[1]
    start = pl.multiple_of(d * hid_w, hid_w)
    quarter = g_v.shape[0] // 4
    wide_loads, down_loads = [], []
    for c in range(4):
        rows = pl.ds(c * quarter, quarter)
        wide_loads.append(pltpu.make_async_copy(w_gate.at[layer, rows, pl.ds(start, hid_w)], g_v.at[rows, :], wsem.at[c]))
        wide_loads.append(pltpu.make_async_copy(w_up.at[layer, rows, pl.ds(start, hid_w)], u_v.at[rows, :], wsem.at[4 + c]))
    for c in range(4):
        rows = hid_w // 4
        down_loads.append(pltpu.make_async_copy(w_down.at[layer, pl.ds(start + c * rows, rows), :], d_v.at[pl.ds(c * rows, rows), :], wsem.at[8 + c]))
    wide_loads[0].start()

    dim = x_v.shape[1]
    own = x_v.shape[0]
    chunks = 4
    wide = dim // chunks

    def send(axis, peer, src, dst, ssem, rsem, i):
        cp = pltpu.make_async_remote_copy(src_ref=src, dst_ref=dst, send_sem=ssem.at[i], recv_sem=rsem.at[i], device_id={axis: peer}, device_id_type=MESH)
        cp.start()
        return cp

    pl.semaphore_wait(barrier, n_tp + n_dp - 2)
    for cp in ins:
        cp.wait()
    rs, gx, fx, xx = [], [], [], []
    for c in range(chunks):
        cols = pl.ds(c * wide, wide)
        for k, p in enumerate(tp_peers):
            rs.append(send("tp", p, part_v.at[p, :, cols], rs_buf.at[k, :, cols], s_rs, r_rs, c * (n_tp - 1) + k))
    for cp in wide_loads[1:5]:
        cp.start()
    for c in range(chunks):
        cols = slice(c * wide, (c + 1) * wide)
        tot = part_v[z, :, cols]
        for k in range(n_tp - 1):
            rs[c * (n_tp - 1) + k].wait_recv()
            tot = tot + rs_buf[k, :, cols]
        xm = (x_v[:, cols].astype(F32) + tot).astype(BF16)
        xm_s[:, cols] = xm.astype(F32)
        g_all[0, :, cols] = xm
        if c % 2 == 1:
            both = pl.ds((c - 1) * wide, 2 * wide)
            for k, p in enumerate(dp_peers):
                gx.append(send("dp", p, g_all.at[0, :, both], g_all.at[k + 1, :, both], s_g, r_g, c // 2 * (n_dp - 1) + k))
        if c < 3:
            wide_loads[5 + c].start()
    for cp in down_loads:
        cp.start()
    for cp in gx:
        cp.wait_recv()
    mids = jnp.concatenate([g_all[k].astype(F32) for k in range(n_dp)], axis=0)
    full = rms(mids, gain_v[layer:layer + 1, :])

    for cp in wide_loads:
        cp.wait()
    tile = 256
    for j in range(hid_w // tile):
        gate = mm(full, g_v[:, j * tile:(j + 1) * tile])
        up = mm(full, u_v[:, j * tile:(j + 1) * tile])
        hid[:, j * tile:(j + 1) * tile] = (gate * jax.nn.sigmoid(gate) * up).astype(BF16)
    for cp in down_loads:
        cp.wait()
    hv = hid[...]
    chunks, wide = 2, dim // 2
    for c in range(chunks):
        y = mm(hv, d_v[:, c * wide:(c + 1) * wide])
        for b in range(n_dp):
            f_snd[b, :, c * wide:(c + 1) * wide] = y[b * own:(b + 1) * own].astype(BF16)
        cols = pl.ds(c * wide, wide)
        for k, p in enumerate(dp_peers):
            fx.append(send("dp", p, f_snd.at[n_dp - 1 - k, :, cols], f_buf.at[k, :, cols], s_f, r_f, c * (n_dp - 1) + k))
    for c in range(chunks):
        cols = slice(c * wide, (c + 1) * wide)
        tot = f_snd[0, :, cols].astype(F32)
        for k in range(n_dp - 1):
            fx[c * (n_dp - 1) + k].wait_recv()
            tot = tot + f_buf[k, :, cols].astype(F32)
        x_new = (xm_s[:, cols] + tot).astype(BF16)
        x_snd[:, cols] = x_new
        out_ref[z, :, cols] = x_new
        for k, p in enumerate(tp_peers):
            xx.append(send("tp", p, x_snd.at[:, pl.ds(c * wide, wide)], out_ref.at[z, :, pl.ds(c * wide, wide)], s_x, r_x, c * (n_tp - 1) + k))
    for cp in xx:
        cp.wait_recv()
    for cp in rs + gx + fx + xx:
        cp.wait_send()


def ffn_call(layer, n_tp, n_dp, part, x, ffn_gain, w_gate, w_up, w_down):
    any_spec = pl.BlockSpec(memory_space=pl.ANY)
    vmem = pl.BlockSpec(memory_space=pltpu.VMEM)
    rows, dim = x.shape
    own = rows // n_tp
    hid_w = w_gate.shape[2] // n_dp
    dma = pltpu.SemaphoreType.DMA
    sends = dma((4 * (n_tp - 1),))
    out = pl.pallas_call(
        functools.partial(ffn_kernel, layer, n_tp, n_dp),
        out_shape=jax.ShapeDtypeStruct((n_tp, own, dim), BF16),
        in_specs=[any_spec] * 6,
        out_specs=vmem,
        scratch_shapes=[
            pltpu.VMEM((n_tp, own, dim), F32),
            pltpu.VMEM((own, dim), BF16),
            pltpu.VMEM(ffn_gain.shape, F32),
            pltpu.VMEM((dim, hid_w), BF16),
            pltpu.VMEM((dim, hid_w), BF16),
            pltpu.VMEM((hid_w, dim), BF16),
            pltpu.VMEM((n_tp - 1, own, dim), F32),
            pltpu.VMEM((own, dim), F32),
            pltpu.VMEM((n_dp, own, dim), BF16),
            pltpu.VMEM((own * n_dp, hid_w), BF16),
            pltpu.VMEM((n_dp, own, dim), BF16),
            pltpu.VMEM((n_dp - 1, own, dim), BF16),
            pltpu.VMEM((own, dim), BF16),
            dma((3,)), dma((12,)), sends, sends, sends, sends, sends, sends, sends, sends,
        ],
        compiler_params=pltpu.CompilerParams(vmem_limit_bytes=VMEM_LIMIT, collective_id=layer, has_side_effects=True),
        cost_estimate=pl.CostEstimate(flops=1_100_000_000, bytes_accessed=35_000_000, transcendentals=0),
        name=f"ffn{layer}",
    )(part.reshape(n_tp, own, dim), x.reshape(n_tp, own, dim), ffn_gain, w_gate, w_up, w_down)
    return out.reshape(rows, dim)


def solution(mesh):
    n_tp = mesh.shape["tp"]
    n_dp = mesh.shape["dp"]
    row_spec = P(("rep", "dp"), None)
    cache_spec = P(("rep", "dp"), None, None)
    in_specs = (row_spec, P(("rep", "dp")), cache_spec, cache_spec, P(), P(), P(), P(), P(), P(), P(None, None, "tp"), P(None, "tp", None, None), P(None, "tp", None, None), P(None, "tp", None), P(), P(), P())
    out_specs = (row_spec, cache_spec, cache_spec)

    def local_step(x, lengths, cache0, cache1, attn_gain, kv_gain, q_gain, ffn_gain, w_dkv, w_qa, w_qb, w_uk, w_uv, w_o, w_gate, w_up, w_down):
        w_dkv_t = jnp.swapaxes(w_dkv, 1, 2)
        new_caches = []
        for layer, cache in enumerate((cache0, cache1)):
            part, new_cache = attn_call(layer, x, lengths, attn_gain, kv_gain, q_gain, jnp.swapaxes(cache, 1, 2), w_dkv_t, w_qa, w_qb, w_uk, w_uv, w_o)
            x = ffn_call(layer, n_tp, n_dp, part, x, ffn_gain, w_gate, w_up, w_down)
            new_caches.append(jnp.swapaxes(new_cache, 1, 2))
        return x, new_caches[0], new_caches[1]

    return jax.shard_map(local_step, mesh=mesh, in_specs=in_specs, out_specs=out_specs, check_vma=False)
```

```python
import functools

import jax
import jax.numpy as jnp
from jax import lax
from jax.experimental import pallas as pl
from jax.experimental.pallas import tpu as pltpu
from jax.sharding import PartitionSpec as P

MESH = pl.DeviceIdType.MESH
EPS = 1e-6
LOG_BASE = 9.210340371976184
F32 = jnp.float32
BF16 = jnp.bfloat16
NT = (((1,), (1,)), ((), ()))
VMEM_LIMIT = 107 * 512 * 1024


def mm(a, b):
    return jnp.dot(a, b, preferred_element_type=F32)


def rms(v, gain):
    inv = lax.rsqrt(jnp.mean(v * v, axis=-1, keepdims=True) + EPS)
    return (v * inv * gain).astype(BF16)


def attn_kernel(layer, x_ref, len_s, len_v, ag_ref, kg_ref, qg_ref, cache, w_dkv, w_qa, w_qb, w_uk, w_uv, w_o, part_ref, out_cache,
                c_v, c_new, dkv_v, qa_v, qb_v, uk_v, uv_v, o_v, qlow_s, ent_f, qs, qb16, sc_s, p_s, os, ho_s, wsem, csem, osem):
    rows, lat, rope, heads, qk = 32, 512, 64, 4, 192
    slots = c_v.shape[2]
    per = 4
    groups = rows // per
    width = 512
    qa_n = qa_v.shape[1] // width
    copies = []
    for n in range(qa_n):
        copies.append(pltpu.make_async_copy(w_qa.at[layer, :, pl.ds(n * width, width)], qa_v.at[:, pl.ds(n * width, width)], wsem.at[n]))
    for i, (src, dst) in enumerate(((w_dkv, dkv_v), (w_qb, qb_v), (w_uk, uk_v), (w_uv, uv_v), (w_o, o_v))):
        copies.append(pltpu.make_async_copy(src.at[layer], dst, wsem.at[qa_n + i]))

    def cache_in(g):
        return pltpu.make_async_copy(cache.at[pl.ds(g * per, per)], c_v.at[pl.ds(g * per, per)], csem.at[g])

    def cache_out(g):
        return pltpu.make_async_copy(c_new.at[pl.ds(g * per, per)], out_cache.at[pl.ds(g * per, per)], osem.at[g])

    for cp in [copies[qa_n]] + copies[:qa_n] + copies[qa_n + 1:qa_n + 3]:
        cp.start()
    for g in range(groups):
        cache_in(g).start()
    copies[qa_n + 3].start()
    copies[qa_n + 4].start()

    xf = x_ref[...].astype(F32)
    h = rms(xf, ag_ref[layer:layer + 1, :])

    half = rope // 2
    lens_row = len_v[...].astype(F32)
    freq_t = jnp.exp(lax.broadcasted_iota(jnp.int32, (half, rows), 0).astype(F32) * (-LOG_BASE / half))
    ang_t = freq_t * jnp.broadcast_to(lens_row, (half, rows))
    cos_t, sin_t = jnp.cos(ang_t), jnp.sin(ang_t)
    cos_r, sin_r = cos_t.T, sin_t.T

    copies[qa_n].wait()
    cut = (lat + rope) // 2
    kt = jnp.concatenate([lax.dot_general(dkv_v[0:cut], h, NT, preferred_element_type=F32), lax.dot_general(dkv_v[cut:], h, NT, preferred_element_type=F32)], axis=0)
    kl = kt[:lat]
    inv_k = lax.rsqrt(jnp.mean(kl * kl, axis=0, keepdims=True) + EPS)
    gain_t = jnp.broadcast_to(kg_ref[layer:layer + 1, :], (128, lat)).T[:, :rows]
    ent_f[0:lat, 0:rows] = (kl * inv_k * gain_t).astype(BF16).astype(F32)
    ka, kb = kt[lat:lat + half], kt[lat + half:]
    ent_f[lat:lat + half, 0:rows] = (ka * cos_t - kb * sin_t).astype(BF16).astype(F32)
    ent_f[lat + half:, 0:rows] = (kb * cos_t + ka * sin_t).astype(BF16).astype(F32)

    ssq = jnp.zeros((rows, 1), F32)
    for n in range(qa_n):
        copies[n].wait()
        part = mm(h, qa_v[:, n * width:(n + 1) * width])
        ssq = ssq + jnp.sum(part * part, axis=-1, keepdims=True)
        qlow_s[:, n * width:(n + 1) * width] = part
    inv_q = lax.rsqrt(ssq / (qa_n * width) + EPS)
    copies[qa_n + 1].wait()
    q_low = (qlow_s[...] * inv_q * qg_ref[layer:layer + 1, :]).astype(BF16)
    q_full = mm(q_low, qb_v[...])
    copies[qa_n + 2].wait()
    for hd in range(heads):
        qh = q_full[:, hd * qk:(hd + 1) * qk]
        q_lat = mm(qh[:, :128].astype(BF16), uk_v[hd])
        for c in range(lat // 128):
            qs[c, pl.ds(hd, rows, stride=heads), :] = q_lat[:, c * 128:(c + 1) * 128]
        qa, qb = qh[:, 128:128 + half], qh[:, 128 + half:]
        rot = jnp.concatenate([qa * cos_r - qb * sin_r, qb * cos_r + qa * sin_r, jnp.zeros((rows, 128 - rope), F32)], axis=-1)
        qs[lat // 128, pl.ds(hd, rows, stride=heads), :] = rot
    for c in range(lat // 128 + 1):
        qb16[:, c * 128:(c + 1) * 128] = qs[c].astype(BF16)

    lane = lax.broadcasted_iota(jnp.int32, (1, slots), 1)
    row_w = lax.broadcasted_iota(jnp.int32, (per * heads, slots), 0) // heads
    row_l = lax.broadcasted_iota(jnp.int32, (per * heads, lat), 0) // heads
    scale = float(qk) ** -0.5

    def insert(g):
        for i in range(per):
            r = g * per + i
            col = jnp.broadcast_to(ent_f[:, r:r + 1], (lat + rope, 128)).astype(BF16)
            hit = jnp.broadcast_to(lane == len_s[r], (lat + rope, slots))
            c_new[r] = jnp.where(hit, jnp.concatenate([col, col], axis=-1), c_v[r])
        cache_out(g).start()

    pairs = rows * heads
    ent = ent_f[:, 0:rows].astype(BF16)
    mine_all = lax.broadcasted_iota(jnp.int32, (pairs, rows), 0) // heads == lax.broadcasted_iota(jnp.int32, (pairs, rows), 1)
    s_new_all = jnp.sum(jnp.where(mine_all, mm(qb16[:, 0:lat + rope], ent), 0.0), axis=-1, keepdims=True) * scale
    len_all = jnp.sum(jnp.where(mine_all, jnp.broadcast_to(lens_row, (pairs, rows)), 0.0), axis=-1, keepdims=True)
    parts = 2
    span = pairs // parts
    lane_p = lax.broadcasted_iota(jnp.int32, (span, slots), 1).astype(F32)
    for t in range(parts):
        block = range(t * groups // parts, (t + 1) * groups // parts)
        for g in block:
            if g % 2 == 0:
                cache_in(g).wait()
                cache_in(g + 1).wait()
            q16 = qb16[g * 16:(g + 1) * 16, 0:lat + rope]
            acc = None
            for i in range(per):
                s_i = mm(q16, c_v[g * per + i])
                acc = s_i if acc is None else jnp.where(row_w == i, s_i, acc)
            sc_s[g * 16:(g + 1) * 16, :] = acc
            insert(g)
        lo, hi = t * span, (t + 1) * span
        s_new, len_p, mine = s_new_all[lo:hi], len_all[lo:hi], mine_all[lo:hi]
        s = jnp.where(lane_p < len_p, sc_s[lo:hi, :] * scale, -1e30)
        top = jnp.maximum(jnp.max(s, axis=-1, keepdims=True), s_new)
        e = jnp.exp(s - top)
        e_new = jnp.exp(s_new - top)
        total = jnp.sum(e, axis=-1, keepdims=True) + e_new
        p_s[lo:hi, :] = jnp.where(lane_p < len_p, e / total, 0.0).astype(BF16)
        p_new = jnp.where(mine, jnp.broadcast_to(e_new / total, (span, rows)), 0.0).astype(BF16)
        o_new = lax.dot_general(p_new, ent[0:lat], NT, preferred_element_type=F32)
        for c in range(lat // 128):
            os[c, lo:hi, :] = o_new[:, c * 128:(c + 1) * 128]
        for g in block:
            p16 = p_s[g * 16:(g + 1) * 16, :]
            acc = None
            for i in range(per):
                o_i = lax.dot_general(p16, c_v[g * per + i, 0:lat, :], NT, preferred_element_type=F32)
                acc = o_i if acc is None else jnp.where(row_l == i, o_i, acc)
            for c in range(lat // 128):
                os[c, g * 16:(g + 1) * 16, :] += acc[:, c * 128:(c + 1) * 128]
    copies[qa_n + 3].wait()
    for hd in range(heads):
        o_lat = jnp.concatenate([os[c, pl.ds(hd, rows, stride=heads), :].astype(BF16) for c in range(lat // 128)], axis=-1)
        ho_s[:, hd * 128:(hd + 1) * 128] = mm(o_lat, uv_v[hd]).astype(BF16)
    copies[qa_n + 4].wait()
    ho = ho_s[...]
    for n in range(4):
        part_ref[:, n * 512:(n + 1) * 512] = mm(ho, o_v[:, n * 512:(n + 1) * 512])
    for g in range(groups):
        cache_out(g).wait()


def attn_call(layer, x, lengths, attn_gain, kv_gain, q_gain, cache_t, w_dkv_t, w_qa, w_qb, w_uk, w_uv, w_o):
    hbm = pl.BlockSpec(memory_space=pltpu.HBM)
    vmem = pl.BlockSpec(memory_space=pltpu.VMEM)
    smem = pl.BlockSpec(memory_space=pltpu.SMEM)
    rows, width, slots = cache_t.shape
    heads = w_uk.shape[1]
    return pl.pallas_call(
        functools.partial(attn_kernel, layer),
        out_shape=(jax.ShapeDtypeStruct(x.shape, F32), jax.ShapeDtypeStruct(cache_t.shape, BF16)),
        in_specs=[vmem, smem, vmem, vmem, vmem, vmem] + [hbm] * 7,
        out_specs=(vmem, hbm),
        scratch_shapes=[
            pltpu.VMEM(cache_t.shape, BF16),
            pltpu.VMEM(cache_t.shape, BF16),
            pltpu.VMEM(w_dkv_t.shape[1:], BF16),
            pltpu.VMEM(w_qa.shape[1:], BF16),
            pltpu.VMEM(w_qb.shape[1:], BF16),
            pltpu.VMEM(w_uk.shape[1:], BF16),
            pltpu.VMEM(w_uv.shape[1:], BF16),
            pltpu.VMEM(w_o.shape[1:], BF16),
            pltpu.VMEM((rows, w_qa.shape[2]), F32),
            pltpu.VMEM((width, 128), F32),
            pltpu.VMEM((5, rows * heads, 128), F32),
            pltpu.VMEM((rows * heads, 640), BF16),
            pltpu.VMEM((rows * heads, slots), F32),
            pltpu.VMEM((rows * heads, slots), BF16),
            pltpu.VMEM((4, rows * heads, 128), F32),
            pltpu.VMEM((rows, heads * 128), BF16),
            pltpu.SemaphoreType.DMA((8,)),
            pltpu.SemaphoreType.DMA((8,)),
            pltpu.SemaphoreType.DMA((8,)),
        ],
        compiler_params=pltpu.CompilerParams(vmem_limit_bytes=VMEM_LIMIT),
        cost_estimate=pl.CostEstimate(flops=2_000_000_000, bytes_accessed=33_000_000, transcendentals=0),
        name=f"attn{layer}",
    )(x, lengths, lengths.reshape(1, rows), attn_gain, kv_gain, q_gain, cache_t, w_dkv_t, w_qa, w_qb, w_uk, w_uv, w_o)


def ffn_kernel(layer, n_tp, n_dp, part, x, gain, w_gate, w_up, w_down, out_ref,
               part_v, x_v, gain_v, g_v, u_v, d_v, rs_buf, xm_s, g_all, hid, f_snd, f_buf, x_snd,
               isem, wsem, s_rs, r_rs, s_g, r_g, s_f, r_f, s_x, r_x):
    z = lax.axis_index("tp")
    d = lax.axis_index("dp")
    tp_peers = [lax.rem(z + k, n_tp) for k in range(1, n_tp)]
    dp_peers = [lax.rem(d + k, n_dp) for k in range(1, n_dp)]
    barrier = pltpu.get_barrier_semaphore()
    for pz in tp_peers:
        pl.semaphore_signal(barrier, inc=1, device_id={"tp": pz}, device_id_type=MESH)
    for pd in dp_peers:
        pl.semaphore_signal(barrier, inc=1, device_id={"dp": pd}, device_id_type=MESH)

    ins = [pltpu.make_async_copy(part, part_v, isem.at[0]), pltpu.make_async_copy(x.at[z], x_v, isem.at[1]), pltpu.make_async_copy(gain, gain_v, isem.at[2])]
    for cp in ins:
        cp.start()
    hid_w = g_v.shape[1]
    start = pl.multiple_of(d * hid_w, hid_w)
    quarter = g_v.shape[0] // 4
    wide_loads, down_loads = [], []
    for c in range(4):
        rows = pl.ds(c * quarter, quarter)
        wide_loads.append(pltpu.make_async_copy(w_gate.at[layer, rows, pl.ds(start, hid_w)], g_v.at[rows, :], wsem.at[c]))
        wide_loads.append(pltpu.make_async_copy(w_up.at[layer, rows, pl.ds(start, hid_w)], u_v.at[rows, :], wsem.at[4 + c]))
    for c in range(4):
        rows = hid_w // 4
        down_loads.append(pltpu.make_async_copy(w_down.at[layer, pl.ds(start + c * rows, rows), :], d_v.at[pl.ds(c * rows, rows), :], wsem.at[8 + c]))
    wide_loads[0].start()

    dim = x_v.shape[1]
    own = x_v.shape[0]
    chunks = 4
    wide = dim // chunks

    def send(axis, peer, src, dst, ssem, rsem, i):
        cp = pltpu.make_async_remote_copy(src_ref=src, dst_ref=dst, send_sem=ssem.at[i], recv_sem=rsem.at[i], device_id={axis: peer}, device_id_type=MESH)
        cp.start()
        return cp

    pl.semaphore_wait(barrier, n_tp + n_dp - 2)
    for cp in ins:
        cp.wait()
    rs, gx, fx, xx = [], [], [], []
    for c in range(chunks):
        cols = pl.ds(c * wide, wide)
        for k, p in enumerate(tp_peers):
            rs.append(send("tp", p, part_v.at[p, :, cols], rs_buf.at[k, :, cols], s_rs, r_rs, c * (n_tp - 1) + k))
    for cp in wide_loads[1:5]:
        cp.start()
    for c in range(chunks):
        cols = slice(c * wide, (c + 1) * wide)
        tot = part_v[z, :, cols]
        for k in range(n_tp - 1):
            rs[c * (n_tp - 1) + k].wait_recv()
            tot = tot + rs_buf[k, :, cols]
        xm = (x_v[:, cols].astype(F32) + tot).astype(BF16)
        xm_s[:, cols] = xm.astype(F32)
        g_all[0, :, cols] = xm
        if c % 2 == 1:
            both = pl.ds((c - 1) * wide, 2 * wide)
            for k, p in enumerate(dp_peers):
                gx.append(send("dp", p, g_all.at[0, :, both], g_all.at[k + 1, :, both], s_g, r_g, c // 2 * (n_dp - 1) + k))
        if c < 3:
            wide_loads[5 + c].start()
    for cp in down_loads:
        cp.start()
    for cp in gx:
        cp.wait_recv()
    mids = jnp.concatenate([g_all[k].astype(F32) for k in range(n_dp)], axis=0)
    full = rms(mids, gain_v[layer:layer + 1, :])

    for cp in wide_loads:
        cp.wait()
    tile = 256
    for j in range(hid_w // tile):
        gate = mm(full, g_v[:, j * tile:(j + 1) * tile])
        up = mm(full, u_v[:, j * tile:(j + 1) * tile])
        hid[:, j * tile:(j + 1) * tile] = (gate * jax.nn.sigmoid(gate) * up).astype(BF16)
    for cp in down_loads:
        cp.wait()
    hv = hid[...]
    chunks, wide = 2, dim // 2
    for c in range(chunks):
        y = mm(hv, d_v[:, c * wide:(c + 1) * wide])
        for b in range(n_dp):
            f_snd[b, :, c * wide:(c + 1) * wide] = y[b * own:(b + 1) * own].astype(BF16)
        cols = pl.ds(c * wide, wide)
        for k, p in enumerate(dp_peers):
            fx.append(send("dp", p, f_snd.at[n_dp - 1 - k, :, cols], f_buf.at[k, :, cols], s_f, r_f, c * (n_dp - 1) + k))
    for c in range(chunks):
        cols = slice(c * wide, (c + 1) * wide)
        tot = f_snd[0, :, cols].astype(F32)
        for k in range(n_dp - 1):
            fx[c * (n_dp - 1) + k].wait_recv()
            tot = tot + f_buf[k, :, cols].astype(F32)
        x_new = (xm_s[:, cols] + tot).astype(BF16)
        x_snd[:, cols] = x_new
        out_ref[z, :, cols] = x_new
        for k, p in enumerate(tp_peers):
            xx.append(send("tp", p, x_snd.at[:, pl.ds(c * wide, wide)], out_ref.at[z, :, pl.ds(c * wide, wide)], s_x, r_x, c * (n_tp - 1) + k))
    for cp in xx:
        cp.wait_recv()
    for cp in rs + gx + fx + xx:
        cp.wait_send()


def ffn_call(layer, n_tp, n_dp, part, x, ffn_gain, w_gate, w_up, w_down):
    any_spec = pl.BlockSpec(memory_space=pl.ANY)
    hbm = pl.BlockSpec(memory_space=pltpu.HBM)
    vmem = pl.BlockSpec(memory_space=pltpu.VMEM)
    rows, dim = x.shape
    own = rows // n_tp
    hid_w = w_gate.shape[2] // n_dp
    dma = pltpu.SemaphoreType.DMA
    sends = dma((4 * (n_tp - 1),))
    out = pl.pallas_call(
        functools.partial(ffn_kernel, layer, n_tp, n_dp),
        out_shape=jax.ShapeDtypeStruct((n_tp, own, dim), BF16),
        in_specs=[any_spec] * 3 + [hbm] * 3,
        out_specs=vmem,
        scratch_shapes=[
            pltpu.VMEM((n_tp, own, dim), F32),
            pltpu.VMEM((own, dim), BF16),
            pltpu.VMEM(ffn_gain.shape, F32),
            pltpu.VMEM((dim, hid_w), BF16),
            pltpu.VMEM((dim, hid_w), BF16),
            pltpu.VMEM((hid_w, dim), BF16),
            pltpu.VMEM((n_tp - 1, own, dim), F32),
            pltpu.VMEM((own, dim), F32),
            pltpu.VMEM((n_dp, own, dim), BF16),
            pltpu.VMEM((own * n_dp, hid_w), BF16),
            pltpu.VMEM((n_dp, own, dim), BF16),
            pltpu.VMEM((n_dp - 1, own, dim), BF16),
            pltpu.VMEM((own, dim), BF16),
            dma((3,)), dma((12,)), sends, sends, sends, sends, sends, sends, sends, sends,
        ],
        compiler_params=pltpu.CompilerParams(vmem_limit_bytes=VMEM_LIMIT, collective_id=layer, has_side_effects=True),
        cost_estimate=pl.CostEstimate(flops=1_100_000_000, bytes_accessed=35_000_000, transcendentals=0),
        name=f"ffn{layer}",
    )(part.reshape(n_tp, own, dim), x.reshape(n_tp, own, dim), ffn_gain, w_gate, w_up, w_down)
    return out.reshape(rows, dim)


def solution(mesh):
    n_tp = mesh.shape["tp"]
    n_dp = mesh.shape["dp"]
    row_spec = P(("rep", "dp"), None)
    cache_spec = P(("rep", "dp"), None, None)
    in_specs = (row_spec, P(("rep", "dp")), cache_spec, cache_spec, P(), P(), P(), P(), P(), P(), P(None, None, "tp"), P(None, "tp", None, None), P(None, "tp", None, None), P(None, "tp", None), P(), P(), P())
    out_specs = (row_spec, cache_spec, cache_spec)

    def local_step(x, lengths, cache0, cache1, attn_gain, kv_gain, q_gain, ffn_gain, w_dkv, w_qa, w_qb, w_uk, w_uv, w_o, w_gate, w_up, w_down):
        w_dkv_t = jnp.swapaxes(w_dkv, 1, 2)
        new_caches = []
        for layer, cache in enumerate((cache0, cache1)):
            part, new_cache = attn_call(layer, x, lengths, attn_gain, kv_gain, q_gain, jnp.swapaxes(cache, 1, 2), w_dkv_t, w_qa, w_qb, w_uk, w_uv, w_o)
            x = ffn_call(layer, n_tp, n_dp, part, x, ffn_gain, w_gate, w_up, w_down)
            new_caches.append(jnp.swapaxes(new_cache, 1, 2))
        return x, new_caches[0], new_caches[1]

    return jax.shard_map(local_step, mesh=mesh, in_specs=in_specs, out_specs=out_specs, check_vma=False)
```

```python
import functools

import jax
import jax.numpy as jnp
from jax import lax
from jax.experimental import pallas as pl
from jax.experimental.pallas import tpu as pltpu
from jax.sharding import PartitionSpec as P

MESH = pl.DeviceIdType.MESH
EPS = 1e-6
LOG_BASE = 9.210340371976184
F32 = jnp.float32
BF16 = jnp.bfloat16
NT = (((1,), (1,)), ((), ()))
VMEM_LIMIT = 107 * 512 * 1024
FULL_VMEM = 60 * 1024 * 1024


def mm(a, b):
    return jnp.dot(a, b, preferred_element_type=F32)


def rms(v, gain):
    inv = lax.rsqrt(jnp.mean(v * v, axis=-1, keepdims=True) + EPS)
    return (v * inv * gain).astype(BF16)


def attn_kernel(layer, x_ref, len_s, len_v, ag_ref, kg_ref, qg_ref, cache, w_dkv, w_qa, w_qb, w_uk, w_uv, w_o, part_ref, out_cache,
                c_v, c_new, dkv_v, qa_v, qb_v, uk_v, uv_v, o_v, qlow_s, ent_f, qs, qb16, sc_s, p_s, os, ho_s, wsem, csem, osem):
    rows, lat, rope, heads, qk = 32, 512, 64, 4, 192
    slots = c_v.shape[2]
    per = 4
    groups = rows // per
    width = 512
    qa_n = qa_v.shape[1] // width
    copies = []
    for n in range(qa_n):
        copies.append(pltpu.make_async_copy(w_qa.at[layer, :, pl.ds(n * width, width)], qa_v.at[:, pl.ds(n * width, width)], wsem.at[n]))
    for i, (src, dst) in enumerate(((w_dkv, dkv_v), (w_qb, qb_v), (w_uk, uk_v), (w_uv, uv_v), (w_o, o_v))):
        copies.append(pltpu.make_async_copy(src.at[layer], dst, wsem.at[qa_n + i]))

    def cache_in(g):
        return pltpu.make_async_copy(cache.at[pl.ds(g * per, per)], c_v.at[pl.ds(g * per, per)], csem.at[g])

    def cache_out(g):
        return pltpu.make_async_copy(c_new.at[pl.ds(g * per, per)], out_cache.at[pl.ds(g * per, per)], osem.at[g])

    for cp in [copies[qa_n]] + copies[:qa_n] + copies[qa_n + 1:qa_n + 3]:
        cp.start()
    for g in range(groups):
        cache_in(g).start()
    copies[qa_n + 3].start()
    copies[qa_n + 4].start()

    xf = x_ref[...].astype(F32)
    h = rms(xf, ag_ref[layer:layer + 1, :])

    half = rope // 2
    lens_row = len_v[...].astype(F32)
    freq_t = jnp.exp(lax.broadcasted_iota(jnp.int32, (half, rows), 0).astype(F32) * (-LOG_BASE / half))
    ang_t = freq_t * jnp.broadcast_to(lens_row, (half, rows))
    cos_t, sin_t = jnp.cos(ang_t), jnp.sin(ang_t)
    cos_r, sin_r = cos_t.T, sin_t.T

    copies[qa_n].wait()
    cut = (lat + rope) // 2
    kt = jnp.concatenate([lax.dot_general(dkv_v[0:cut], h, NT, preferred_element_type=F32), lax.dot_general(dkv_v[cut:], h, NT, preferred_element_type=F32)], axis=0)
    kl = kt[:lat]
    inv_k = lax.rsqrt(jnp.mean(kl * kl, axis=0, keepdims=True) + EPS)
    gain_t = jnp.broadcast_to(kg_ref[layer:layer + 1, :], (128, lat)).T[:, :rows]
    ent_f[0:lat, 0:rows] = (kl * inv_k * gain_t).astype(BF16).astype(F32)
    ka, kb = kt[lat:lat + half], kt[lat + half:]
    ent_f[lat:lat + half, 0:rows] = (ka * cos_t - kb * sin_t).astype(BF16).astype(F32)
    ent_f[lat + half:, 0:rows] = (kb * cos_t + ka * sin_t).astype(BF16).astype(F32)

    ssq = jnp.zeros((rows, 1), F32)
    for n in range(qa_n):
        copies[n].wait()
        part = mm(h, qa_v[:, n * width:(n + 1) * width])
        ssq = ssq + jnp.sum(part * part, axis=-1, keepdims=True)
        qlow_s[:, n * width:(n + 1) * width] = part
    inv_q = lax.rsqrt(ssq / (qa_n * width) + EPS)
    copies[qa_n + 1].wait()
    q_low = (qlow_s[...] * inv_q * qg_ref[layer:layer + 1, :]).astype(BF16)
    q_full = mm(q_low, qb_v[...])
    copies[qa_n + 2].wait()
    for hd in range(heads):
        qh = q_full[:, hd * qk:(hd + 1) * qk]
        q_lat = mm(qh[:, :128].astype(BF16), uk_v[hd])
        for c in range(lat // 128):
            qs[c, pl.ds(hd, rows, stride=heads), :] = q_lat[:, c * 128:(c + 1) * 128]
        qa, qb = qh[:, 128:128 + half], qh[:, 128 + half:]
        rot = jnp.concatenate([qa * cos_r - qb * sin_r, qb * cos_r + qa * sin_r, jnp.zeros((rows, 128 - rope), F32)], axis=-1)
        qs[lat // 128, pl.ds(hd, rows, stride=heads), :] = rot
    for c in range(lat // 128 + 1):
        qb16[:, c * 128:(c + 1) * 128] = qs[c].astype(BF16)

    lane = lax.broadcasted_iota(jnp.int32, (1, slots), 1)
    row_w = lax.broadcasted_iota(jnp.int32, (per * heads, slots), 0) // heads
    row_l = lax.broadcasted_iota(jnp.int32, (per * heads, lat), 0) // heads
    scale = float(qk) ** -0.5

    def insert(g):
        for i in range(per):
            r = g * per + i
            col = jnp.broadcast_to(ent_f[:, r:r + 1], (lat + rope, 128)).astype(BF16)
            hit = jnp.broadcast_to(lane == len_s[r], (lat + rope, slots))
            c_new[r] = jnp.where(hit, jnp.concatenate([col, col], axis=-1), c_v[r])
        cache_out(g).start()

    pairs = rows * heads
    ent = ent_f[:, 0:rows].astype(BF16)
    mine_all = lax.broadcasted_iota(jnp.int32, (pairs, rows), 0) // heads == lax.broadcasted_iota(jnp.int32, (pairs, rows), 1)
    s_new_all = jnp.sum(jnp.where(mine_all, mm(qb16[:, 0:lat + rope], ent), 0.0), axis=-1, keepdims=True) * scale
    len_all = jnp.sum(jnp.where(mine_all, jnp.broadcast_to(lens_row, (pairs, rows)), 0.0), axis=-1, keepdims=True)
    parts = 2
    span = pairs // parts
    lane_p = lax.broadcasted_iota(jnp.int32, (span, slots), 1).astype(F32)
    for t in range(parts):
        block = range(t * groups // parts, (t + 1) * groups // parts)
        for g in block:
            if g % 2 == 0:
                cache_in(g).wait()
                cache_in(g + 1).wait()
            q16 = qb16[g * 16:(g + 1) * 16, 0:lat + rope]
            acc = None
            for i in range(per):
                s_i = mm(q16, c_v[g * per + i])
                acc = s_i if acc is None else jnp.where(row_w == i, s_i, acc)
            sc_s[g * 16:(g + 1) * 16, :] = acc
            insert(g)
        lo, hi = t * span, (t + 1) * span
        s_new, len_p, mine = s_new_all[lo:hi], len_all[lo:hi], mine_all[lo:hi]
        s = jnp.where(lane_p < len_p, sc_s[lo:hi, :] * scale, -1e30)
        top = jnp.maximum(jnp.max(s, axis=-1, keepdims=True), s_new)
        e = jnp.exp(s - top)
        e_new = jnp.exp(s_new - top)
        total = jnp.sum(e, axis=-1, keepdims=True) + e_new
        p_s[lo:hi, :] = jnp.where(lane_p < len_p, e / total, 0.0).astype(BF16)
        p_new = jnp.where(mine, jnp.broadcast_to(e_new / total, (span, rows)), 0.0).astype(BF16)
        o_new = lax.dot_general(p_new, ent[0:lat], NT, preferred_element_type=F32)
        for c in range(lat // 128):
            os[c, lo:hi, :] = o_new[:, c * 128:(c + 1) * 128]
        for g in block:
            p16 = p_s[g * 16:(g + 1) * 16, :]
            acc = None
            for i in range(per):
                o_i = lax.dot_general(p16, c_v[g * per + i, 0:lat, :], NT, preferred_element_type=F32)
                acc = o_i if acc is None else jnp.where(row_l == i, o_i, acc)
            for c in range(lat // 128):
                os[c, g * 16:(g + 1) * 16, :] += acc[:, c * 128:(c + 1) * 128]
    copies[qa_n + 3].wait()
    for hd in range(heads):
        o_lat = jnp.concatenate([os[c, pl.ds(hd, rows, stride=heads), :].astype(BF16) for c in range(lat // 128)], axis=-1)
        ho_s[:, hd * 128:(hd + 1) * 128] = mm(o_lat, uv_v[hd]).astype(BF16)
    copies[qa_n + 4].wait()
    ho = ho_s[...]
    for n in range(4):
        part_ref[:, n * 512:(n + 1) * 512] = mm(ho, o_v[:, n * 512:(n + 1) * 512])
    for g in range(groups):
        cache_out(g).wait()


def attn_call(layer, x, lengths, attn_gain, kv_gain, q_gain, cache_t, w_dkv_t, w_qa, w_qb, w_uk, w_uv, w_o):
    hbm = pl.BlockSpec(memory_space=pltpu.HBM)
    vmem = pl.BlockSpec(memory_space=pltpu.VMEM)
    smem = pl.BlockSpec(memory_space=pltpu.SMEM)
    rows, width, slots = cache_t.shape
    heads = w_uk.shape[1]
    return pl.pallas_call(
        functools.partial(attn_kernel, layer),
        out_shape=(jax.ShapeDtypeStruct(x.shape, F32), jax.ShapeDtypeStruct(cache_t.shape, BF16)),
        in_specs=[vmem, smem, vmem, vmem, vmem, vmem] + [hbm] * 7,
        out_specs=(vmem, hbm),
        scratch_shapes=[
            pltpu.VMEM(cache_t.shape, BF16),
            pltpu.VMEM(cache_t.shape, BF16),
            pltpu.VMEM(w_dkv_t.shape[1:], BF16),
            pltpu.VMEM(w_qa.shape[1:], BF16),
            pltpu.VMEM(w_qb.shape[1:], BF16),
            pltpu.VMEM(w_uk.shape[1:], BF16),
            pltpu.VMEM(w_uv.shape[1:], BF16),
            pltpu.VMEM(w_o.shape[1:], BF16),
            pltpu.VMEM((rows, w_qa.shape[2]), F32),
            pltpu.VMEM((width, 128), F32),
            pltpu.VMEM((5, rows * heads, 128), F32),
            pltpu.VMEM((rows * heads, 640), BF16),
            pltpu.VMEM((rows * heads, slots), F32),
            pltpu.VMEM((rows * heads, slots), BF16),
            pltpu.VMEM((4, rows * heads, 128), F32),
            pltpu.VMEM((rows, heads * 128), BF16),
            pltpu.SemaphoreType.DMA((8,)),
            pltpu.SemaphoreType.DMA((8,)),
            pltpu.SemaphoreType.DMA((8,)),
        ],
        compiler_params=pltpu.CompilerParams(vmem_limit_bytes=VMEM_LIMIT if layer else FULL_VMEM),
        cost_estimate=pl.CostEstimate(flops=2_000_000_000, bytes_accessed=33_000_000, transcendentals=0),
        name=f"attn{layer}",
    )(x, lengths, lengths.reshape(1, rows), attn_gain, kv_gain, q_gain, cache_t, w_dkv_t, w_qa, w_qb, w_uk, w_uv, w_o)


def ffn_kernel(layer, n_tp, n_dp, part, x, gain, w_gate, w_up, w_down, out_ref,
               part_v, x_v, gain_v, g_v, u_v, d_v, rs_buf, xm_s, g_all, hid, f_snd, f_buf, x_snd,
               isem, wsem, s_rs, r_rs, s_g, r_g, s_f, r_f, s_x, r_x):
    z = lax.axis_index("tp")
    d = lax.axis_index("dp")
    tp_peers = [lax.rem(z + k, n_tp) for k in range(1, n_tp)]
    dp_peers = [lax.rem(d + k, n_dp) for k in range(1, n_dp)]
    barrier = pltpu.get_barrier_semaphore()
    for pz in tp_peers:
        pl.semaphore_signal(barrier, inc=1, device_id={"tp": pz}, device_id_type=MESH)
    for pd in dp_peers:
        pl.semaphore_signal(barrier, inc=1, device_id={"dp": pd}, device_id_type=MESH)

    ins = [pltpu.make_async_copy(part, part_v, isem.at[0]), pltpu.make_async_copy(x.at[z], x_v, isem.at[1]), pltpu.make_async_copy(gain, gain_v, isem.at[2])]
    for cp in ins:
        cp.start()
    hid_w = g_v.shape[1]
    start = pl.multiple_of(d * hid_w, hid_w)
    quarter = g_v.shape[0] // 4
    wide_loads, down_loads = [], []
    for c in range(4):
        rows = pl.ds(c * quarter, quarter)
        wide_loads.append(pltpu.make_async_copy(w_gate.at[layer, rows, pl.ds(start, hid_w)], g_v.at[rows, :], wsem.at[c]))
        wide_loads.append(pltpu.make_async_copy(w_up.at[layer, rows, pl.ds(start, hid_w)], u_v.at[rows, :], wsem.at[4 + c]))
    for c in range(4):
        rows = hid_w // 4
        down_loads.append(pltpu.make_async_copy(w_down.at[layer, pl.ds(start + c * rows, rows), :], d_v.at[pl.ds(c * rows, rows), :], wsem.at[8 + c]))
    wide_loads[0].start()

    dim = x_v.shape[1]
    own = x_v.shape[0]
    chunks = 4
    wide = dim // chunks

    def send(axis, peer, src, dst, ssem, rsem, i):
        cp = pltpu.make_async_remote_copy(src_ref=src, dst_ref=dst, send_sem=ssem.at[i], recv_sem=rsem.at[i], device_id={axis: peer}, device_id_type=MESH)
        cp.start()
        return cp

    pl.semaphore_wait(barrier, n_tp + n_dp - 2)
    for cp in ins:
        cp.wait()
    rs, gx, fx, xx = [], [], [], []
    for c in range(chunks):
        cols = pl.ds(c * wide, wide)
        for k, p in enumerate(tp_peers):
            rs.append(send("tp", p, part_v.at[p, :, cols], rs_buf.at[k, :, cols], s_rs, r_rs, c * (n_tp - 1) + k))
    for cp in wide_loads[1:5]:
        cp.start()
    for c in range(chunks):
        cols = slice(c * wide, (c + 1) * wide)
        tot = part_v[z, :, cols]
        for k in range(n_tp - 1):
            rs[c * (n_tp - 1) + k].wait_recv()
            tot = tot + rs_buf[k, :, cols]
        xm = (x_v[:, cols].astype(F32) + tot).astype(BF16)
        xm_s[:, cols] = xm.astype(F32)
        g_all[0, :, cols] = xm
        if c % 2 == 1:
            both = pl.ds((c - 1) * wide, 2 * wide)
            for k, p in enumerate(dp_peers):
                gx.append(send("dp", p, g_all.at[0, :, both], g_all.at[k + 1, :, both], s_g, r_g, c // 2 * (n_dp - 1) + k))
        if c < 3:
            wide_loads[5 + c].start()
    for cp in down_loads:
        cp.start()
    for cp in gx:
        cp.wait_recv()
    mids = jnp.concatenate([g_all[k].astype(F32) for k in range(n_dp)], axis=0)
    full = rms(mids, gain_v[layer:layer + 1, :])

    for cp in wide_loads:
        cp.wait()
    tile = 256
    for j in range(hid_w // tile):
        gate = mm(full, g_v[:, j * tile:(j + 1) * tile])
        up = mm(full, u_v[:, j * tile:(j + 1) * tile])
        hid[:, j * tile:(j + 1) * tile] = (gate * jax.nn.sigmoid(gate) * up).astype(BF16)
    for cp in down_loads:
        cp.wait()
    hv = hid[...]
    chunks, wide = 2, dim // 2
    for c in range(chunks):
        y = mm(hv, d_v[:, c * wide:(c + 1) * wide])
        for b in range(n_dp):
            f_snd[b, :, c * wide:(c + 1) * wide] = y[b * own:(b + 1) * own].astype(BF16)
        cols = pl.ds(c * wide, wide)
        for k, p in enumerate(dp_peers):
            fx.append(send("dp", p, f_snd.at[n_dp - 1 - k, :, cols], f_buf.at[k, :, cols], s_f, r_f, c * (n_dp - 1) + k))
    for c in range(chunks):
        cols = slice(c * wide, (c + 1) * wide)
        tot = f_snd[0, :, cols].astype(F32)
        for k in range(n_dp - 1):
            fx[c * (n_dp - 1) + k].wait_recv()
            tot = tot + f_buf[k, :, cols].astype(F32)
        x_new = (xm_s[:, cols] + tot).astype(BF16)
        x_snd[:, cols] = x_new
        out_ref[z, :, cols] = x_new
        for k, p in enumerate(tp_peers):
            xx.append(send("tp", p, x_snd.at[:, pl.ds(c * wide, wide)], out_ref.at[z, :, pl.ds(c * wide, wide)], s_x, r_x, c * (n_tp - 1) + k))
    for cp in xx:
        cp.wait_recv()
    for cp in rs + gx + fx + xx:
        cp.wait_send()


def ffn_call(layer, n_tp, n_dp, part, x, ffn_gain, w_gate, w_up, w_down):
    any_spec = pl.BlockSpec(memory_space=pl.ANY)
    hbm = pl.BlockSpec(memory_space=pltpu.HBM)
    vmem = pl.BlockSpec(memory_space=pltpu.VMEM)
    rows, dim = x.shape
    own = rows // n_tp
    hid_w = w_gate.shape[2] // n_dp
    dma = pltpu.SemaphoreType.DMA
    sends = dma((4 * (n_tp - 1),))
    out = pl.pallas_call(
        functools.partial(ffn_kernel, layer, n_tp, n_dp),
        out_shape=jax.ShapeDtypeStruct((n_tp, own, dim), BF16),
        in_specs=[any_spec] * 3 + [hbm] * 3,
        out_specs=vmem,
        scratch_shapes=[
            pltpu.VMEM((n_tp, own, dim), F32),
            pltpu.VMEM((own, dim), BF16),
            pltpu.VMEM(ffn_gain.shape, F32),
            pltpu.VMEM((dim, hid_w), BF16),
            pltpu.VMEM((dim, hid_w), BF16),
            pltpu.VMEM((hid_w, dim), BF16),
            pltpu.VMEM((n_tp - 1, own, dim), F32),
            pltpu.VMEM((own, dim), F32),
            pltpu.VMEM((n_dp, own, dim), BF16),
            pltpu.VMEM((own * n_dp, hid_w), BF16),
            pltpu.VMEM((n_dp, own, dim), BF16),
            pltpu.VMEM((n_dp - 1, own, dim), BF16),
            pltpu.VMEM((own, dim), BF16),
            dma((3,)), dma((12,)), sends, sends, sends, sends, sends, sends, sends, sends,
        ],
        compiler_params=pltpu.CompilerParams(vmem_limit_bytes=VMEM_LIMIT, collective_id=layer, has_side_effects=True),
        cost_estimate=pl.CostEstimate(flops=1_100_000_000, bytes_accessed=35_000_000, transcendentals=0),
        name=f"ffn{layer}",
    )(part.reshape(n_tp, own, dim), x.reshape(n_tp, own, dim), ffn_gain, w_gate, w_up, w_down)
    return out.reshape(rows, dim)


def solution(mesh):
    n_tp = mesh.shape["tp"]
    n_dp = mesh.shape["dp"]
    row_spec = P(("rep", "dp"), None)
    cache_spec = P(("rep", "dp"), None, None)
    in_specs = (row_spec, P(("rep", "dp")), cache_spec, cache_spec, P(), P(), P(), P(), P(), P(), P(None, None, "tp"), P(None, "tp", None, None), P(None, "tp", None, None), P(None, "tp", None), P(), P(), P())
    out_specs = (row_spec, cache_spec, cache_spec)

    def local_step(x, lengths, cache0, cache1, attn_gain, kv_gain, q_gain, ffn_gain, w_dkv, w_qa, w_qb, w_uk, w_uv, w_o, w_gate, w_up, w_down):
        w_dkv_t = jnp.swapaxes(w_dkv, 1, 2)
        new_caches = []
        for layer, cache in enumerate((cache0, cache1)):
            part, new_cache = attn_call(layer, x, lengths, attn_gain, kv_gain, q_gain, jnp.swapaxes(cache, 1, 2), w_dkv_t, w_qa, w_qb, w_uk, w_uv, w_o)
            x = ffn_call(layer, n_tp, n_dp, part, x, ffn_gain, w_gate, w_up, w_down)
            new_caches.append(jnp.swapaxes(new_cache, 1, 2))
        return x, new_caches[0], new_caches[1]

    return jax.shard_map(local_step, mesh=mesh, in_specs=in_specs, out_specs=out_specs, check_vma=False)
```
